32 devices in a mesh: gx: 4 (over y, x), gy: 4 (over z), gz: 2 (over core).
Axes of the slice: x: 2, y: 2, z: 4, core: 2. Of those that a mesh axis runs over, the one named last changes fastest.
Arguments:
- density: float32 [32, 256, 256], P('gx', 'gy', 'gz'), may hold values from 0.2 to 6, as said below
- momentum: float32 [3, 32, 256, 256], P(None, 'gx', 'gy', 'gz'), may hold values from -6 to 6
- energy: float32 [32, 256, 256], P('gx', 'gy', 'gz'), may hold values from 0.2 to 6, as said below
- displacement: int32 [3, 32, 256, 256], P(None, 'gx', 'gy', 'gz'), may hold values from -255 to 255
- flags: int32 [6], replicated, may hold values from 0 to 1
Outputs:
- new_density: float32 [32, 256, 256], P('gx', 'gy', 'gz')
- new_momentum: float32 [3, 32, 256, 256], P(None, 'gx', 'gy', 'gz')
- new_energy: float32 [32, 256, 256], P('gx', 'gy', 'gz')
- totals: float32 [2], replicated
The draws below stay inside these ranges and needn't reach their ends.
Inputs may be any that keep to these rules, and one draw needn't show every extreme that they name: density is positive. energy is positive.
All inputs are finite; a program needn't handle non-finite values.
Results may differ from the reference program's by a relative error of at most 0.0003.
Values sent between devices are 32-bit elements; how exact they have to be, the bound alone decides.
A program may use at most 64 MiB of HBM per device.

```python
import jax
import jax.numpy as jnp
from jax import lax

NX = 32
NY = 256
NZ = 256


def rising_field(key):
    uniform_part = jax.random.uniform(key, (NX, NY, NZ), jnp.float32)
    ramp = 1.0 + 2.0 * jnp.arange(NX, dtype=jnp.float32)[:, None, None] / NX
    base = 0.5 + uniform_part
    return base * ramp


def draw_density(key, part):
    return rising_field(jax.random.fold_in(key, 11))


def draw_energy(key, part):
    return rising_field(jax.random.fold_in(key, 23))


def with_ends(entries, own_key, least, largest):
    shape = entries.shape
    spot = [jax.random.randint(jax.random.fold_in(own_key, axis), (), 0, shape[axis]) for axis in range(len(shape))]
    entries = entries.at[tuple(spot)].set(least)
    longest = shape.index(max(shape))
    spot[longest] = (spot[longest] + 1) % shape[longest]
    return entries.at[tuple(spot)].set(largest)


def shard_levels(key, shape, cuts, least, largest):
    level = 1.0
    for position, shards_of in cuts:
        draws = jax.random.uniform(jax.random.fold_in(jax.random.fold_in(key, 6), position), (shards_of,), jnp.float32, least / len(cuts), largest / len(cuts))
        level = level * jnp.repeat(jnp.exp(draws), shape[position] // shards_of).reshape((-1,) + (1,) * (len(shape) - 1 - position))
    return level


def centred(key, extent, spread, bound, split=(), held_as=jnp.bfloat16):
    level = shard_levels(key, extent, split, -0.22, 0.18) if split else 1.0
    values = jax.random.normal(key, extent, jnp.float32) * spread * level
    return jnp.minimum(jnp.maximum(values, -bound), bound).astype(held_as)


def setup_inputs(seed: int = 0) -> dict:
    streams_of = jax.random.split(jax.random.key(seed), 6)
    return {
        "density": draw_density(jax.random.fold_in(streams_of[5], 71), 0),
        "momentum": centred(streams_of[1], (3, NX, NY, NZ), 1.0, 6.0, ((1, 4), (2, 4), (3, 2)), jnp.float32),
        "energy": draw_energy(jax.random.fold_in(streams_of[5], 71), 0),
        "displacement": with_ends(jax.random.randint(streams_of[3], (3, NX, NY, NZ), -255, 256), jax.random.fold_in(streams_of[3], 1), -255, 255).astype(jnp.int32),
        "flags": with_ends(jax.random.randint(streams_of[4], (6,), 0, 2), jax.random.fold_in(streams_of[4], 1), 0, 1).astype(jnp.int32),
    }


def minmod(left_diff, right_diff):
    return 0.5 * (jnp.sign(left_diff) + jnp.sign(right_diff)) * jnp.minimum(jnp.abs(left_diff), jnp.abs(right_diff))


def flux_change(padded, face_rows, along):
    total_len = padded.shape[along]
    upper_cells = lax.slice_in_dim(padded, 2, total_len, axis=along)
    middle = lax.slice_in_dim(padded, 1, total_len - 1, axis=along)
    lower_cells = lax.slice_in_dim(padded, 0, total_len - 2, axis=along)
    slopes = minmod(upper_cells - middle, middle - lower_cells)
    k = total_len - 2
    low_val = lax.slice_in_dim(middle, 0, k - 1, axis=along)
    high_val = lax.slice_in_dim(middle, 1, k, axis=along)
    low_slope = lax.slice_in_dim(slopes, 0, k - 1, axis=along)
    high_slope = lax.slice_in_dim(slopes, 1, k, axis=along)
    fluxes = face_rows * jnp.where(face_rows > 0, low_val + 0.5 * (1.0 - face_rows) * low_slope,
                                   high_val - 0.5 * (1.0 + face_rows) * high_slope)
    m = k - 1
    return lax.slice_in_dim(fluxes, 0, m - 1, axis=along) - lax.slice_in_dim(fluxes, 1, m, axis=along)


def axis_change(values, face_speed, low_flag, high_flag, along):
    n = values.shape[along]
    first_cell = lax.slice_in_dim(values, 0, 1, axis=along)
    last_cell = lax.slice_in_dim(values, n - 1, n, axis=along)
    padded = jnp.concatenate([first_cell, first_cell, values, last_cell, last_cell], along)
    face_rows = jnp.concatenate([lax.slice_in_dim(face_speed, 0, 1, axis=along) * low_flag,
                                 lax.slice_in_dim(face_speed, 1, n, axis=along),
                                 lax.slice_in_dim(face_speed, n - 1, n, axis=along) * high_flag], along)
    return flux_change(padded, face_rows, along)


def reference(density, momentum, energy, displacement, flags):
    face_speed = displacement.astype(jnp.float32) / 256.0
    flag_open = flags.astype(jnp.float32)

    def remap_field(values):
        updated = values
        for along in range(3):
            updated = updated + axis_change(values, face_speed[along], flag_open[2 * along], flag_open[2 * along + 1], along)
        return updated

    new_density = remap_field(density)
    new_momentum = jnp.stack([remap_field(momentum[comp]) for comp in range(3)])
    new_energy = remap_field(energy)
    cell_total = float(NX * NY * NZ)
    totals = jnp.stack([jnp.sum(new_density), jnp.sum(new_energy)]) / cell_total
    return new_density, new_momentum, new_energy, totals
```

```python
import functools

import jax
import jax.numpy as jnp
from jax import lax
from jax.experimental import pallas as pl
from jax.experimental.pallas import tpu as pltpu
from jax.sharding import PartitionSpec as P

AXES = ("gx", "gy", "gz")
SUB = 8


def minmod(p, r):
    return jnp.maximum(jnp.minimum(r, 0.0), jnp.minimum(p, jnp.maximum(r, 0.0)))


def gain(v):
    size = jnp.abs(v)
    return 0.5 * size * (1.0 - size)


def flux(v, g, q_low, q_high, s_low, s_high):
    up = v > 0
    return v * jnp.where(up, q_low, q_high) + g * jnp.where(up, s_low, s_high)


def kernel(
    sizes, flags, den, mom, en, disp, out_d, out_m, out_e, totals,
    q, dx, dy, dz, xlo, xhi, xv, edge, zlo, zhi, cq, cs, sum_x, sum_y, sum_z,
    local_sem, send_sem, recv_sem, ssx, rsx, ssy, rsy, ssz, rsz,
):
    nx, ny, nz = den.shape
    pos = {a: lax.axis_index(a) for a in AXES}
    top = ny + SUB
    per = nz // 4
    parts = edge.shape[0]
    scale = 1.0 / 256.0
    cells = float(nx * ny * nz)
    for a in AXES:
        cells = cells * sizes[a]

    locals_ = [
        pltpu.make_async_copy(den, q.at[0, :, SUB:top], local_sem.at[0]),
        pltpu.make_async_copy(mom, q.at[1:4, :, SUB:top], local_sem.at[1]),
        pltpu.make_async_copy(en, q.at[4, :, SUB:top], local_sem.at[2]),
        pltpu.make_async_copy(disp.at[2], dz, local_sem.at[3]),
        pltpu.make_async_copy(disp.at[1], dy.at[:, SUB:top], local_sem.at[4]),
        pltpu.make_async_copy(disp.at[0], dx, local_sem.at[5]),
    ]
    for c in locals_:
        c.start()

    barrier = pltpu.get_barrier_semaphore()
    greeted = 0
    for a in AXES:
        for o in range(1, sizes[a]):
            peer = lax.rem(pos[a] + o, sizes[a])
            pl.semaphore_signal(
                barrier, inc=1, device_id={a: peer}, device_id_type=pl.DeviceIdType.MESH
            )
            greeted += 1
    pl.semaphore_wait(barrier, greeted)

    def copy(k, src, dst, axis, step):
        return pltpu.make_async_remote_copy(
            src_ref=src, dst_ref=dst, send_sem=send_sem.at[k], recv_sem=recv_sem.at[k],
            device_id={axis: pos[axis] + step}, device_id_type=pl.DeviceIdType.MESH,
        )

    last = {a: sizes[a] - 1 for a in AXES}
    x_up = [
        copy(0, den.at[nx - 2 : nx], xlo.at[0], "gx", 1),
        copy(1, mom.at[:, nx - 2 : nx], xlo.at[1:4], "gx", 1),
        copy(2, en.at[nx - 2 : nx], xlo.at[4], "gx", 1),
    ]
    x_down = [
        copy(3, den.at[0:2], xhi.at[0], "gx", -1),
        copy(4, mom.at[:, 0:2], xhi.at[1:4], "gx", -1),
        copy(5, en.at[0:2], xhi.at[4], "gx", -1),
        copy(6, disp.at[0, 0], xv, "gx", -1),
    ]
    hi_rows = slice(top, top + SUB)
    y_up = [
        copy(7, den.at[:, ny - SUB : ny], q.at[0, :, 0:SUB], "gy", 1),
        copy(8, mom.at[:, :, ny - SUB : ny], q.at[1:4, :, 0:SUB], "gy", 1),
        copy(9, en.at[:, ny - SUB : ny], q.at[4, :, 0:SUB], "gy", 1),
    ]
    y_down = [
        copy(10, den.at[:, 0:SUB], q.at[0, :, hi_rows], "gy", -1),
        copy(11, mom.at[:, :, 0:SUB], q.at[1:4, :, hi_rows], "gy", -1),
        copy(12, en.at[:, 0:SUB], q.at[4, :, hi_rows], "gy", -1),
        copy(13, disp.at[1, :, 0:SUB], dy.at[:, hi_rows], "gy", -1),
    ]
    z_up = [copy(14, edge, zlo, "gz", 1)]
    z_down = [copy(15, edge, zhi, "gz", -1)]

    def start(axis, ups, downs):
        @pl.when(pos[axis] < last[axis])
        def _():
            for c in ups:
                c.start()

        @pl.when(pos[axis] > 0)
        def _():
            for c in downs:
                c.start()

    def arrive(axis, ups, downs, fill_low, fill_high):
        @pl.when(pos[axis] > 0)
        def _():
            for c in ups:
                c.wait_recv()

        @pl.when(pos[axis] < last[axis])
        def _():
            for c in downs:
                c.wait_recv()

        @pl.when(pos[axis] == 0)
        def _():
            fill_low()

        @pl.when(pos[axis] == last[axis])
        def _():
            fill_high()

    def sent(axis, ups, downs):
        @pl.when(pos[axis] < last[axis])
        def _():
            for c in ups:
                c.wait_send()

        @pl.when(pos[axis] > 0)
        def _():
            for c in downs:
                c.wait_send()

    start("gx", x_up, x_down)
    start("gy", y_up, y_down)

    flag = [flags[i].astype(jnp.float32) for i in range(6)]

    def low_mult(a):
        return jnp.where(pos[AXES[a]] == 0, flag[2 * a], 1.0)

    def high_mult(a):
        return jnp.where(pos[AXES[a]] == last[AXES[a]], flag[2 * a + 1], 1.0)

    def outer_low(a):
        return jnp.where(pos[AXES[a]] == 0, flag[2 * a], 0.0)

    def outer_high(a):
        return jnp.where(pos[AXES[a]] == last[AXES[a]], flag[2 * a + 1], 0.0)

    for c in locals_:
        c.wait()

    lane = lax.broadcasted_iota(jnp.int32, (ny, nz), 1)
    row = lax.broadcasted_iota(jnp.int32, (ny, nz), 0)

    def pack(x, carry):
        new = list(carry)
        for f in range(6):
            p = f * nx + x
            k = f * nx // per
            at = 4 * lax.rem(p, per)
            plane = q[f, x, SUB:top] if f < 5 else dz[x].astype(jnp.float32)
            moved = pltpu.roll(plane, at, 1)
            mine = lax.rem(lane + 2 - at + nz, nz) < 4
            new[k] = jnp.where(mine, moved, new[k])
        return tuple(new)

    packed = lax.fori_loop(0, nx, pack, tuple(jnp.zeros((ny, nz), jnp.float32) for _ in range(parts)))
    for k in range(parts):
        edge[k] = packed[k]

    wz = jnp.where(lane == 0, outer_low(2), 0.0) - jnp.where(lane == nz - 1, outer_high(2), 0.0)
    wy = jnp.where(row == 0, outer_low(1), 0.0) - jnp.where(row == ny - 1, outer_high(1), 0.0)
    wx_low, wx_high = outer_low(0), outer_high(0)

    def total(x, carry):
        a, b = carry
        wx = jnp.where(x == 0, wx_low, 0.0) - jnp.where(x == nx - 1, wx_high, 0.0)
        w = 1.0 + scale * (
            wz * dz[x].astype(jnp.float32)
            + wy * dy[x, SUB:top].astype(jnp.float32)
            + wx * dx[x].astype(jnp.float32)
        )
        return (
            a + jnp.sum((q[0, x, SUB:top] * w).reshape(ny // SUB, SUB, nz), 0),
            b + jnp.sum((q[4, x, SUB:top] * w).reshape(ny // SUB, SUB, nz), 0),
        )

    zero = jnp.zeros((SUB, nz), jnp.float32)
    mass, power = lax.fori_loop(0, nx, total, (zero, zero))
    sum_z[pos["gz"], 0] = mass
    sum_z[pos["gz"], 1] = power
    start("gz", z_up, z_down)

    def line(axis, slots, ss, rs):
        count = sizes[axis]
        copies = []
        for o in range(1, count):
            me = pos[axis]
            copies.append(
                pltpu.make_async_remote_copy(
                    src_ref=slots.at[me], dst_ref=slots.at[me], send_sem=ss.at[o],
                    recv_sem=rs.at[me], device_id={axis: lax.rem(me + o, count)},
                    device_id_type=pl.DeviceIdType.MESH,
                )
            )
        return copies

    def collect(axis, slots, ss, rs):
        count = sizes[axis]
        for o in range(1, count):
            peer = lax.rem(pos[axis] + o, count)
            pltpu.make_async_remote_copy(
                src_ref=slots.at[peer], dst_ref=slots.at[peer], send_sem=ss.at[o],
                recv_sem=rs.at[peer], device_id={axis: peer},
                device_id_type=pl.DeviceIdType.MESH,
            ).wait_recv()
        a, b = slots[0, 0], slots[0, 1]
        for o in range(1, count):
            a = a + slots[o, 0]
            b = b + slots[o, 1]
        return a, b

    line_z = line("gz", sum_z, ssz, rsz)
    line_y = line("gy", sum_y, ssy, rsy)
    line_x = line("gx", sum_x, ssx, rsx)
    for c in line_z:
        c.start()

    def z_low():
        e = edge[...]
        zlo[...] = jnp.where(lane3 & 3 == 3, pltpu.roll(e, nz - 1, 2), pltpu.roll(e, nz - 2, 2))

    def z_high():
        e = edge[...]
        zhi[...] = jnp.where(lane3 & 3 == 0, pltpu.roll(e, 1, 2), pltpu.roll(e, 2, 2))

    lane3 = lax.broadcasted_iota(jnp.int32, (parts, ny, nz), 2)
    arrive("gz", z_up, z_down, z_low, z_high)
    low = lane & 3 == 0
    for k in range(parts):
        e, l, h = edge[k], zlo[k], zhi[k]
        r1, r2 = pltpu.roll(l, 1, 1), pltpu.roll(l, 2, 1)
        l1, l2 = pltpu.roll(h, nz - 1, 1), pltpu.roll(h, nz - 2, 1)
        cq[k] = jnp.where(low, r1, l1)
        cs[k] = jnp.where(low, minmod(e - r1, r1 - r2), minmod(l2 - l1, l1 - e))

    first, final = lane == 0, lane == nz - 1
    z_lo_mult = jnp.where(first, low_mult(2), 1.0) * scale
    z_hi_mult = high_mult(2) * scale
    outs = (
        lambda x: out_d.at[x], lambda x: out_m.at[0, x], lambda x: out_m.at[1, x],
        lambda x: out_m.at[2, x], lambda x: out_e.at[x],
    )

    def along_z(x, _):
        v = dz[x].astype(jnp.float32) * z_lo_mult
        g = gain(v)

        def ghosts(ref, f):
            back = lax.rem(nz - 4 * lax.rem(f * nx + x, per), nz)
            return pltpu.roll(ref[f * nx // per], back, 1)

        vh = ghosts(cq, 5) * z_hi_mult
        gh = gain(vh)
        for f in range(5):
            plane = q[f, x, SUB:top]
            gq, gs = ghosts(cq, f), ghosts(cs, f)
            qm = jnp.where(first, gq, pltpu.roll(plane, 1, 1))
            d = plane - qm
            s = minmod(jnp.where(final, gq - plane, pltpu.roll(d, nz - 1, 1)), d)
            sm = jnp.where(first, gs, pltpu.roll(s, 1, 1))
            fl = flux(v, g, qm, plane, sm, s)
            fh = jnp.where(final, flux(vh, gh, plane, gq, s, gs), pltpu.roll(fl, nz - 1, 1))
            outs[f](x)[...] = plane + (fl - fh)
        return 0

    lax.fori_loop(0, nx, along_z, 0)

    a, b = collect("gz", sum_z, ssz, rsz)
    sum_y[pos["gy"], 0] = a
    sum_y[pos["gy"], 1] = b

    def y_low():
        q[:, :, 0:SUB] = jnp.broadcast_to(q[:, :, SUB : SUB + 1], (5, nx, SUB, nz))

    def y_high():
        q[:, :, hi_rows] = jnp.broadcast_to(q[:, :, top - 1 : top], (5, nx, SUB, nz))
        dy[:, hi_rows] = jnp.broadcast_to(dy[:, top - 1 : top], (nx, SUB, nz))

    arrive("gy", y_up, y_down, y_low, y_high)
    for c in line_y:
        c.start()
    tall = ny + 2 * SUB
    rows = lax.broadcasted_iota(jnp.int32, (tall, nz), 0)
    inside = (rows >= SUB) & (rows <= top)
    y_mult = jnp.where(
        rows == SUB, low_mult(1) * scale, jnp.where(rows == top, high_mult(1) * scale, scale)
    )

    def along_y(x, _):
        v = jnp.where(inside, dy[x].astype(jnp.float32), 0.0) * y_mult
        g = gain(v)
        for f in range(5):
            plane = q[f, x]
            qm = pltpu.roll(plane, 1, 0)
            d = plane - qm
            s = minmod(pltpu.roll(d, tall - 1, 0), d)
            fl = flux(v, g, qm, plane, pltpu.roll(s, 1, 0), s)
            ch = fl - pltpu.roll(fl, tall - 1, 0)
            outs[f](x)[...] += ch[SUB:top]
        return 0

    lax.fori_loop(0, nx, along_y, 0)

    a, b = collect("gy", sum_y, ssy, rsy)
    sum_x[pos["gx"], 0] = a
    sum_x[pos["gx"], 1] = b

    def x_low():
        xlo[...] = jnp.broadcast_to(q[:, 0:1, SUB:top], (5, 2, ny, nz))

    def x_high():
        xhi[...] = jnp.broadcast_to(q[:, nx - 1 : nx, SUB:top], (5, 2, ny, nz))
        xv[...] = dx[nx - 1]

    for c in line_x:
        c.start()
    arrive("gx", x_up, x_down, x_low, x_high)
    x_lo_mult, x_hi_mult = low_mult(0) * scale, high_mult(0) * scale

    def along_x(r, _):
        at = pl.ds(pl.multiple_of(r * SUB, SUB), SUB)
        inner = pl.ds(pl.multiple_of(r * SUB + SUB, SUB), SUB)
        vs = [dx[c, at].astype(jnp.float32) * (x_lo_mult if c == 0 else scale) for c in range(nx)]
        vs.append(xv[at].astype(jnp.float32) * x_hi_mult)
        gs = [gain(v) for v in vs]
        for f in range(5):
            line_q = (
                [xlo[f, 0, at], xlo[f, 1, at]]
                + [q[f, c, inner] for c in range(nx)]
                + [xhi[f, 0, at], xhi[f, 1, at]]
            )
            ds = [line_q[i + 1] - line_q[i] for i in range(nx + 3)]
            ss = [minmod(ds[i + 1], ds[i]) for i in range(nx + 2)]
            fl = [
                flux(vs[i], gs[i], line_q[i + 1], line_q[i + 2], ss[i], ss[i + 1])
                for i in range(nx + 1)
            ]
            for c in range(nx):
                ref = outs[f](c)
                ref[at] += fl[c] - fl[c + 1]
        return 0

    lax.fori_loop(0, ny // SUB, along_x, 0)

    a, b = collect("gx", sum_x, ssx, rsx)
    totals[0] = jnp.sum(a) / cells
    totals[1] = jnp.sum(b) / cells
    sent("gx", x_up, x_down)
    sent("gy", y_up, y_down)
    sent("gz", z_up, z_down)
    for c in line_x + line_y + line_z:
        c.wait_send()


def shards(density, momentum, energy, displacement, flags):
    sizes = {a: lax.axis_size(a) for a in AXES}
    nx, ny, nz = density.shape
    tall = ny + 2 * SUB
    per = nz // 4
    parts = -(-6 * nx // per)
    f32, i32 = jnp.float32, jnp.int32
    dma = pltpu.SemaphoreType.DMA
    any_ = pl.BlockSpec(memory_space=pl.ANY)
    vmem = pl.BlockSpec(memory_space=pltpu.VMEM)
    smem = pl.BlockSpec(memory_space=pltpu.SMEM)
    return pl.pallas_call(
        functools.partial(kernel, sizes),
        out_shape=(
            jax.ShapeDtypeStruct(density.shape, f32),
            jax.ShapeDtypeStruct(momentum.shape, f32),
            jax.ShapeDtypeStruct(energy.shape, f32),
            jax.ShapeDtypeStruct((2,), f32),
        ),
        in_specs=[smem, any_, any_, any_, any_],
        out_specs=(vmem, vmem, vmem, smem),
        scratch_shapes=[
            pltpu.VMEM((5, nx, tall, nz), f32),
            pltpu.VMEM((nx, ny, nz), i32),
            pltpu.VMEM((nx, tall, nz), i32),
            pltpu.VMEM((nx, ny, nz), i32),
            pltpu.VMEM((5, 2, ny, nz), f32),
            pltpu.VMEM((5, 2, ny, nz), f32),
            pltpu.VMEM((ny, nz), i32),
        ]
        + [pltpu.VMEM((parts, ny, nz), f32) for _ in range(5)]
        + [pltpu.VMEM((sizes[a], 2, SUB, nz), f32) for a in AXES]
        + [dma((6,)), dma((16,)), dma((16,))]
        + [dma((sizes[a],)) for a in AXES for _ in range(2)],
        compiler_params=pltpu.CompilerParams(collective_id=0, has_side_effects=True),
    )(flags, density, momentum, energy, displacement)


def solution(mesh):
    return jax.shard_map(
        shards,
        mesh=mesh,
        in_specs=(
            P("gx", "gy", "gz"),
            P(None, "gx", "gy", "gz"),
            P("gx", "gy", "gz"),
            P(None, "gx", "gy", "gz"),
            P(),
        ),
        out_specs=(P("gx", "gy", "gz"), P(None, "gx", "gy", "gz"), P("gx", "gy", "gz"), P()),
        check_vma=False,
    )
```

```python
import functools

import jax
import jax.numpy as jnp
from jax import lax
from jax.experimental import pallas as pl
from jax.experimental.pallas import tpu as pltpu
from jax.sharding import PartitionSpec as P

AXES = ("gx", "gy", "gz")
SUB = 8


def minmod(p, r):
    return jnp.maximum(jnp.minimum(r, 0.0), jnp.minimum(p, jnp.maximum(r, 0.0)))


def gain(v):
    size = jnp.abs(v)
    return 0.5 * size * (1.0 - size)


def flux(v, g, q_low, q_high, s_low, s_high):
    up = v > 0
    return v * jnp.where(up, q_low, q_high) + g * jnp.where(up, s_low, s_high)


def kernel(
    sizes, flags, den, mom, en, disp, out_d, out_m, out_e, sums,
    q, dx, dy, dz, xlo, xhi, xv, edge, zlo, zhi, cq, cs, sum_x, sum_y, sum_z,
    local_sem, send_sem, recv_sem, ssx, rsx, ssy, rsy, ssz, rsz,
):
    nx, ny, nz = den.shape
    pos = {a: lax.axis_index(a) for a in AXES}
    top = ny + SUB
    per = nz // 4
    parts = edge.shape[0]
    scale = 1.0 / 256.0

    locals_ = [
        pltpu.make_async_copy(den, q.at[0, :, SUB:top], local_sem.at[0]),
        pltpu.make_async_copy(mom, q.at[1:4, :, SUB:top], local_sem.at[1]),
        pltpu.make_async_copy(en, q.at[4, :, SUB:top], local_sem.at[2]),
        pltpu.make_async_copy(disp.at[2], dz, local_sem.at[3]),
        pltpu.make_async_copy(disp.at[1], dy.at[:, SUB:top], local_sem.at[4]),
        pltpu.make_async_copy(disp.at[0], dx, local_sem.at[5]),
    ]
    for c in locals_:
        c.start()

    barrier = pltpu.get_barrier_semaphore()
    greeted = 0
    for a in AXES:
        for o in range(1, sizes[a]):
            peer = lax.rem(pos[a] + o, sizes[a])
            pl.semaphore_signal(
                barrier, inc=1, device_id={a: peer}, device_id_type=pl.DeviceIdType.MESH
            )
            greeted += 1
    pl.semaphore_wait(barrier, greeted)

    def copy(k, src, dst, axis, step):
        return pltpu.make_async_remote_copy(
            src_ref=src, dst_ref=dst, send_sem=send_sem.at[k], recv_sem=recv_sem.at[k],
            device_id={axis: pos[axis] + step}, device_id_type=pl.DeviceIdType.MESH,
        )

    last = {a: sizes[a] - 1 for a in AXES}
    x_up = [
        copy(0, den.at[nx - 2 : nx], xlo.at[0], "gx", 1),
        copy(1, mom.at[:, nx - 2 : nx], xlo.at[1:4], "gx", 1),
        copy(2, en.at[nx - 2 : nx], xlo.at[4], "gx", 1),
    ]
    x_down = [
        copy(3, den.at[0:2], xhi.at[0], "gx", -1),
        copy(4, mom.at[:, 0:2], xhi.at[1:4], "gx", -1),
        copy(5, en.at[0:2], xhi.at[4], "gx", -1),
        copy(6, disp.at[0, 0], xv, "gx", -1),
    ]
    hi_rows = slice(top, top + SUB)
    y_up = [
        copy(7, den.at[:, ny - SUB : ny], q.at[0, :, 0:SUB], "gy", 1),
        copy(8, mom.at[:, :, ny - SUB : ny], q.at[1:4, :, 0:SUB], "gy", 1),
        copy(9, en.at[:, ny - SUB : ny], q.at[4, :, 0:SUB], "gy", 1),
    ]
    y_down = [
        copy(10, den.at[:, 0:SUB], q.at[0, :, hi_rows], "gy", -1),
        copy(11, mom.at[:, :, 0:SUB], q.at[1:4, :, hi_rows], "gy", -1),
        copy(12, en.at[:, 0:SUB], q.at[4, :, hi_rows], "gy", -1),
        copy(13, disp.at[1, :, 0:SUB], dy.at[:, hi_rows], "gy", -1),
    ]
    z_up = [copy(14, edge, zlo, "gz", 1)]
    z_down = [copy(15, edge, zhi, "gz", -1)]

    def start(axis, ups, downs):
        @pl.when(pos[axis] < last[axis])
        def _():
            for c in ups:
                c.start()

        @pl.when(pos[axis] > 0)
        def _():
            for c in downs:
                c.start()

    def arrive(axis, ups, downs, fill_low, fill_high):
        @pl.when(pos[axis] > 0)
        def _():
            for c in ups:
                c.wait_recv()

        @pl.when(pos[axis] < last[axis])
        def _():
            for c in downs:
                c.wait_recv()

        @pl.when(pos[axis] == 0)
        def _():
            fill_low()

        @pl.when(pos[axis] == last[axis])
        def _():
            fill_high()

    def sent(axis, ups, downs):
        @pl.when(pos[axis] < last[axis])
        def _():
            for c in ups:
                c.wait_send()

        @pl.when(pos[axis] > 0)
        def _():
            for c in downs:
                c.wait_send()

    start("gx", x_up, x_down)
    start("gy", y_up, y_down)

    flag = [flags[i].astype(jnp.float32) for i in range(6)]

    def low_mult(a):
        return jnp.where(pos[AXES[a]] == 0, flag[2 * a], 1.0)

    def high_mult(a):
        return jnp.where(pos[AXES[a]] == last[AXES[a]], flag[2 * a + 1], 1.0)

    def outer_low(a):
        return jnp.where(pos[AXES[a]] == 0, flag[2 * a], 0.0)

    def outer_high(a):
        return jnp.where(pos[AXES[a]] == last[AXES[a]], flag[2 * a + 1], 0.0)

    for c in locals_:
        c.wait()

    lane = lax.broadcasted_iota(jnp.int32, (ny, nz), 1)
    row = lax.broadcasted_iota(jnp.int32, (ny, nz), 0)

    def pack(x, carry):
        new = list(carry)
        for f in range(6):
            p = f * nx + x
            k = f * nx // per
            at = 4 * lax.rem(p, per)
            plane = q[f, x, SUB:top] if f < 5 else dz[x].astype(jnp.float32)
            moved = pltpu.roll(plane, at, 1)
            mine = lax.rem(lane + 2 - at + nz, nz) < 4
            new[k] = jnp.where(mine, moved, new[k])
        return tuple(new)

    packed = lax.fori_loop(0, nx, pack, tuple(jnp.zeros((ny, nz), jnp.float32) for _ in range(parts)))
    for k in range(parts):
        edge[k] = packed[k]

    wz = jnp.where(lane == 0, outer_low(2), 0.0) - jnp.where(lane == nz - 1, outer_high(2), 0.0)
    wy = jnp.where(row == 0, outer_low(1), 0.0) - jnp.where(row == ny - 1, outer_high(1), 0.0)
    wx_low, wx_high = outer_low(0), outer_high(0)

    def total(x, carry):
        a, b = carry
        wx = jnp.where(x == 0, wx_low, 0.0) - jnp.where(x == nx - 1, wx_high, 0.0)
        w = 1.0 + scale * (
            wz * dz[x].astype(jnp.float32)
            + wy * dy[x, SUB:top].astype(jnp.float32)
            + wx * dx[x].astype(jnp.float32)
        )
        return (
            a + jnp.sum((q[0, x, SUB:top] * w).reshape(ny // SUB, SUB, nz), 0),
            b + jnp.sum((q[4, x, SUB:top] * w).reshape(ny // SUB, SUB, nz), 0),
        )

    zero = jnp.zeros((SUB, nz), jnp.float32)
    mass, power = lax.fori_loop(0, nx, total, (zero, zero))
    sum_z[pos["gz"], 0] = mass
    sum_z[pos["gz"], 1] = power
    start("gz", z_up, z_down)

    def line(axis, slots, ss, rs):
        count = sizes[axis]
        copies = []
        for o in range(1, count):
            me = pos[axis]
            copies.append(
                pltpu.make_async_remote_copy(
                    src_ref=slots.at[me], dst_ref=slots.at[me], send_sem=ss.at[o],
                    recv_sem=rs.at[me], device_id={axis: lax.rem(me + o, count)},
                    device_id_type=pl.DeviceIdType.MESH,
                )
            )
        return copies

    def collect(axis, slots, ss, rs):
        count = sizes[axis]
        for o in range(1, count):
            peer = lax.rem(pos[axis] + o, count)
            pltpu.make_async_remote_copy(
                src_ref=slots.at[peer], dst_ref=slots.at[peer], send_sem=ss.at[o],
                recv_sem=rs.at[peer], device_id={axis: peer},
                device_id_type=pl.DeviceIdType.MESH,
            ).wait_recv()
        a, b = slots[0, 0], slots[0, 1]
        for o in range(1, count):
            a = a + slots[o, 0]
            b = b + slots[o, 1]
        return a, b

    line_z = line("gz", sum_z, ssz, rsz)
    line_y = line("gy", sum_y, ssy, rsy)
    line_x = line("gx", sum_x, ssx, rsx)
    for c in line_z:
        c.start()

    def z_low():
        e = edge[...]
        zlo[...] = jnp.where(lane3 & 3 == 3, pltpu.roll(e, nz - 1, 2), pltpu.roll(e, nz - 2, 2))

    def z_high():
        e = edge[...]
        zhi[...] = jnp.where(lane3 & 3 == 0, pltpu.roll(e, 1, 2), pltpu.roll(e, 2, 2))

    lane3 = lax.broadcasted_iota(jnp.int32, (parts, ny, nz), 2)
    arrive("gz", z_up, z_down, z_low, z_high)
    low = lane & 3 == 0
    for k in range(parts):
        e, l, h = edge[k], zlo[k], zhi[k]
        r1, r2 = pltpu.roll(l, 1, 1), pltpu.roll(l, 2, 1)
        l1, l2 = pltpu.roll(h, nz - 1, 1), pltpu.roll(h, nz - 2, 1)
        cq[k] = jnp.where(low, r1, l1)
        cs[k] = jnp.where(low, minmod(e - r1, r1 - r2), minmod(l2 - l1, l1 - e))

    first, final = lane == 0, lane == nz - 1
    z_lo_mult = jnp.where(first, low_mult(2), 1.0) * scale
    z_hi_mult = high_mult(2) * scale
    outs = (
        lambda x: out_d.at[x], lambda x: out_m.at[0, x], lambda x: out_m.at[1, x],
        lambda x: out_m.at[2, x], lambda x: out_e.at[x],
    )

    def along_z(x, _):
        v = dz[x].astype(jnp.float32) * z_lo_mult
        g = gain(v)

        def ghosts(ref, f):
            back = lax.rem(nz - 4 * lax.rem(f * nx + x, per), nz)
            return pltpu.roll(ref[f * nx // per], back, 1)

        vh = ghosts(cq, 5) * z_hi_mult
        gh = gain(vh)
        for f in range(5):
            plane = q[f, x, SUB:top]
            gq, gs = ghosts(cq, f), ghosts(cs, f)
            qm = jnp.where(first, gq, pltpu.roll(plane, 1, 1))
            d = plane - qm
            s = minmod(jnp.where(final, gq - plane, pltpu.roll(d, nz - 1, 1)), d)
            sm = jnp.where(first, gs, pltpu.roll(s, 1, 1))
            fl = flux(v, g, qm, plane, sm, s)
            fh = jnp.where(final, flux(vh, gh, plane, gq, s, gs), pltpu.roll(fl, nz - 1, 1))
            outs[f](x)[...] = plane + (fl - fh)
        return 0

    lax.fori_loop(0, nx, along_z, 0)

    a, b = collect("gz", sum_z, ssz, rsz)
    sum_y[pos["gy"], 0] = a
    sum_y[pos["gy"], 1] = b

    def y_low():
        q[:, :, 0:SUB] = jnp.broadcast_to(q[:, :, SUB : SUB + 1], (5, nx, SUB, nz))

    def y_high():
        q[:, :, hi_rows] = jnp.broadcast_to(q[:, :, top - 1 : top], (5, nx, SUB, nz))
        dy[:, hi_rows] = jnp.broadcast_to(dy[:, top - 1 : top], (nx, SUB, nz))

    arrive("gy", y_up, y_down, y_low, y_high)
    for c in line_y:
        c.start()
    tall = ny + 2 * SUB
    rows = lax.broadcasted_iota(jnp.int32, (tall, nz), 0)
    inside = (rows >= SUB) & (rows <= top)
    y_mult = jnp.where(
        rows == SUB, low_mult(1) * scale, jnp.where(rows == top, high_mult(1) * scale, scale)
    )

    def along_y(x, _):
        v = jnp.where(inside, dy[x].astype(jnp.float32), 0.0) * y_mult
        g = gain(v)
        for f in range(5):
            plane = q[f, x]
            qm = pltpu.roll(plane, 1, 0)
            d = plane - qm
            s = minmod(pltpu.roll(d, tall - 1, 0), d)
            fl = flux(v, g, qm, plane, pltpu.roll(s, 1, 0), s)
            ch = fl - pltpu.roll(fl, tall - 1, 0)
            outs[f](x)[...] += ch[SUB:top]
        return 0

    lax.fori_loop(0, nx, along_y, 0)

    a, b = collect("gy", sum_y, ssy, rsy)
    sum_x[pos["gx"], 0] = a
    sum_x[pos["gx"], 1] = b

    def core(r, _):
        at = pl.ds(pl.multiple_of(r * SUB, SUB), SUB)
        inner = pl.ds(pl.multiple_of(r * SUB + SUB, SUB), SUB)
        vs = [dx[c, at].astype(jnp.float32) * scale for c in range(2, nx - 1)]
        gs = [gain(v) for v in vs]
        for f in range(5):
            line_q = [q[f, c, inner] for c in range(nx)]
            ds = [line_q[i + 1] - line_q[i] for i in range(nx - 1)]
            ss = [minmod(ds[i + 1], ds[i]) for i in range(nx - 2)]
            fl = [
                flux(vs[i], gs[i], line_q[i + 1], line_q[i + 2], ss[i], ss[i + 1])
                for i in range(nx - 3)
            ]
            for c in range(1, nx - 1):
                change = fl[c - 2] if c >= 2 else 0.0
                ref = outs[f](c)
                ref[at] += change - fl[c - 1] if c < nx - 2 else change
        return 0

    lax.fori_loop(0, ny // SUB, core, 0)

    def x_low():
        xlo[...] = jnp.broadcast_to(q[:, 0:1, SUB:top], (5, 2, ny, nz))

    def x_high():
        xhi[...] = jnp.broadcast_to(q[:, nx - 1 : nx, SUB:top], (5, 2, ny, nz))
        xv[...] = dx[nx - 1]

    for c in line_x:
        c.start()
    arrive("gx", x_up, x_down, x_low, x_high)
    x_lo_mult, x_hi_mult = low_mult(0) * scale, high_mult(0) * scale

    def x_rows(r):
        return pl.ds(pl.multiple_of(r * SUB, SUB), SUB), pl.ds(
            pl.multiple_of(r * SUB + SUB, SUB), SUB
        )

    def x_flux(v, g, cells4):
        ds = [cells4[i + 1] - cells4[i] for i in range(3)]
        return flux(
            v, g, cells4[1], cells4[2], minmod(ds[1], ds[0]), minmod(ds[2], ds[1])
        )

    def rim(r, _):
        at, inner = x_rows(r)
        faces = (0, 1, nx - 1, nx)
        vs = [
            dx[0, at].astype(jnp.float32) * x_lo_mult,
            dx[1, at].astype(jnp.float32) * scale,
            dx[nx - 1, at].astype(jnp.float32) * scale,
            xv[at].astype(jnp.float32) * x_hi_mult,
        ]
        gs = [gain(v) for v in vs]
        for f in range(5):
            a = [xlo[f, 0, at], xlo[f, 1, at]] + [q[f, c, inner] for c in range(3)]
            b = [q[f, c, inner] for c in range(nx - 3, nx)] + [xhi[f, 0, at], xhi[f, 1, at]]
            fl = [x_flux(vs[i], gs[i], (a, a, b, b)[i][i % 2 : i % 2 + 4]) for i in range(4)]
            for c, change in (
                (0, fl[0] - fl[1]), (1, fl[1]), (nx - 2, -fl[2]), (nx - 1, fl[2] - fl[3]),
            ):
                ref = outs[f](c)
                ref[at] += change
        return 0

    lax.fori_loop(0, ny // SUB, rim, 0)

    a, b = collect("gx", sum_x, ssx, rsx)
    sums[0] = a
    sums[1] = b
    sent("gx", x_up, x_down)
    sent("gy", y_up, y_down)
    sent("gz", z_up, z_down)
    for c in line_x + line_y + line_z:
        c.wait_send()


def put(cells, den, mom, en, sums, out_d, out_m, out_e, totals, sem):
    moves = [
        pltpu.make_async_copy(src, dst, sem.at[i])
        for i, (src, dst) in enumerate(((mom, out_m), (den, out_d), (en, out_e)))
    ]
    for c in moves:
        c.start()
    totals[0] = jnp.sum(sums[0]) / cells
    totals[1] = jnp.sum(sums[1]) / cells
    for c in moves:
        c.wait()


def shards(density, momentum, energy, displacement, flags):
    sizes = {a: lax.axis_size(a) for a in AXES}
    nx, ny, nz = density.shape
    tall = ny + 2 * SUB
    per = nz // 4
    parts = -(-6 * nx // per)
    f32, i32 = jnp.float32, jnp.int32
    dma = pltpu.SemaphoreType.DMA
    any_ = pl.BlockSpec(memory_space=pl.ANY)
    hbm = pl.BlockSpec(memory_space=pltpu.HBM)
    vmem = pl.BlockSpec(memory_space=pltpu.VMEM)
    smem = pl.BlockSpec(memory_space=pltpu.SMEM)
    cells = float(nx * ny * nz)
    for a in AXES:
        cells = cells * sizes[a]
    outputs = tuple(jax.ShapeDtypeStruct(v.shape, f32) for v in (density, momentum, energy))
    results = pl.pallas_call(
        functools.partial(kernel, sizes),
        out_shape=outputs + (jax.ShapeDtypeStruct((2, SUB, nz), f32),),
        in_specs=[smem, hbm, hbm, hbm, hbm],
        out_specs=(vmem, vmem, vmem, vmem),
        scratch_shapes=[
            pltpu.VMEM((5, nx, tall, nz), f32),
            pltpu.VMEM((nx, ny, nz), i32),
            pltpu.VMEM((nx, tall, nz), i32),
            pltpu.VMEM((nx, ny, nz), i32),
            pltpu.VMEM((5, 2, ny, nz), f32),
            pltpu.VMEM((5, 2, ny, nz), f32),
            pltpu.VMEM((ny, nz), i32),
        ]
        + [pltpu.VMEM((parts, ny, nz), f32) for _ in range(5)]
        + [pltpu.VMEM((sizes[a], 2, SUB, nz), f32) for a in AXES]
        + [dma((6,)), dma((16,)), dma((16,))]
        + [dma((sizes[a],)) for a in AXES for _ in range(2)],
        compiler_params=pltpu.CompilerParams(
            collective_id=0, has_side_effects=True, vmem_limit_bytes=12 << 20
        ),
    )(flags, *(pltpu.with_memory_space_constraint(v, pltpu.HBM) for v in (density, momentum, energy, displacement)))
    return pl.pallas_call(
        functools.partial(put, cells),
        out_shape=outputs + (jax.ShapeDtypeStruct((2,), f32),),
        in_specs=[any_, any_, any_, vmem],
        out_specs=(hbm, hbm, hbm, smem),
        scratch_shapes=[dma((3,))],
        compiler_params=pltpu.CompilerParams(vmem_limit_bytes=2 << 20),
    )(*results)


def solution(mesh):
    return jax.shard_map(
        shards,
        mesh=mesh,
        in_specs=(
            P("gx", "gy", "gz"),
            P(None, "gx", "gy", "gz"),
            P("gx", "gy", "gz"),
            P(None, "gx", "gy", "gz"),
            P(),
        ),
        out_specs=(P("gx", "gy", "gz"), P(None, "gx", "gy", "gz"), P("gx", "gy", "gz"), P()),
        check_vma=False,
    )
```

```python
import functools

import jax
import jax.numpy as jnp
from jax import lax
from jax.experimental import pallas as pl
from jax.experimental.pallas import tpu as pltpu
from jax.sharding import PartitionSpec as P

AXES = ("gx", "gy", "gz")
SUB = 8


def minmod(p, r):
    return jnp.maximum(jnp.minimum(r, 0.0), jnp.minimum(p, jnp.maximum(r, 0.0)))


def gain(v):
    size = jnp.abs(v)
    return 0.5 * size * (1.0 - size)


def flux(v, g, q_low, q_high, s_low, s_high):
    up = v > 0
    return v * jnp.where(up, q_low, q_high) + g * jnp.where(up, s_low, s_high)


def kernel(
    sizes, flags_in, den, mom, en, disp, out_d, out_m, out_e, sums,
    flags, q, dx, dy, dz, xh, hop, xv, edge, zlo, zhi, cq, cs, sum_x, sum_y, sum_z,
    local_sem, send_sem, recv_sem, ssx, rsx, ssy, rsy, ssz, rsz,
):
    nx, ny, nz = den.shape
    pos = {a: lax.axis_index(a) for a in AXES}
    top = ny + SUB
    per = nz // 4
    parts = edge.shape[0]
    scale = 1.0 / 256.0
    xlo, xhi = xh.at[0], xh.at[1]

    locals_ = [
        pltpu.make_async_copy(den, q.at[0, :, SUB:top], local_sem.at[0]),
        pltpu.make_async_copy(mom, q.at[1:4, :, SUB:top], local_sem.at[1]),
        pltpu.make_async_copy(en, q.at[4, :, SUB:top], local_sem.at[2]),
        pltpu.make_async_copy(disp.at[2], dz, local_sem.at[3]),
        pltpu.make_async_copy(disp.at[1], dy.at[:, SUB:top], local_sem.at[4]),
        pltpu.make_async_copy(disp.at[0], dx, local_sem.at[5]),
        pltpu.make_async_copy(flags_in, flags, local_sem.at[6]),
    ]
    for c in locals_:
        c.start()

    barrier = pltpu.get_barrier_semaphore()
    greeted = 0
    for a in AXES:
        for o in range(1, sizes[a]):
            peer = lax.rem(pos[a] + o, sizes[a])
            pl.semaphore_signal(
                barrier, inc=1, device_id={a: peer}, device_id_type=pl.DeviceIdType.MESH
            )
            greeted += 1
    pl.semaphore_wait(barrier, greeted)

    def copy(k, src, dst, axis, step):
        return pltpu.make_async_remote_copy(
            src_ref=src, dst_ref=dst, send_sem=send_sem.at[k], recv_sem=recv_sem.at[k],
            device_id={axis: pos[axis] + step}, device_id_type=pl.DeviceIdType.MESH,
        )

    last = {a: sizes[a] - 1 for a in AXES}
    me = pos["gx"]
    par = lax.rem(me, 2)
    odd = par == 1
    end = last["gx"]
    leg_out = (odd & (me + 2 <= end)) | ((par == 0) & (me >= 2))
    relays = (odd & (me >= 3)) | ((par == 0) & (me + 2 <= end))
    leg_in = (me + 1 <= end) & (odd | (me >= 2))
    begin = par * (nx - 2)
    other = 1 - par

    def remote(k, src, dst, target):
        return pltpu.make_async_remote_copy(
            src_ref=src, dst_ref=dst, send_sem=send_sem.at[k], recv_sem=recv_sem.at[k],
            device_id={"gx": target}, device_id_type=pl.DeviceIdType.MESH,
        )

    over = me + 4 * par - 2
    legs = [
        remote(16, mom.at[0, pl.ds(begin, 2)], hop.at[0:2], over),
        remote(17, mom.at[1, pl.ds(begin, 2)], hop.at[2:4], over),
        remote(18, en.at[begin], hop.at[4], over),
    ]
    beside = me + 1 - 2 * par
    onward = [
        remote(19, hop.at[0:2], xh.at[other, 1], beside),
        remote(20, hop.at[2:4], xh.at[other, 2], beside),
        remote(21, hop.at[4], xh.at[other, 4, 0], beside),
    ]
    landed = [
        remote(19, hop.at[0:2], xh.at[par, 1], beside),
        remote(20, hop.at[2:4], xh.at[par, 2], beside),
        remote(21, hop.at[4], xh.at[par, 4, 0], beside),
    ]
    x_up = [
        copy(0, den.at[nx - 2 : nx], xlo.at[0], "gx", 1),
        copy(1, mom.at[2, nx - 2 : nx], xlo.at[3], "gx", 1),
        copy(2, en.at[nx - 1], xlo.at[4, 1], "gx", 1),
    ]
    x_up_half = [
        copy(22, mom.at[0:2, nx - 2 : nx], xlo.at[1:3], "gx", 1),
        copy(23, en.at[nx - 2], xlo.at[4, 0], "gx", 1),
    ]
    x_down = [
        copy(6, disp.at[0, 0], xv, "gx", -1),
        copy(3, den.at[0:2], xhi.at[0], "gx", -1),
        copy(4, mom.at[2, 0:2], xhi.at[3], "gx", -1),
        copy(5, en.at[1], xhi.at[4, 1], "gx", -1),
    ]
    x_down_half = [
        copy(24, mom.at[0:2, 0:2], xhi.at[1:3], "gx", -1),
        copy(25, en.at[0], xhi.at[4, 0], "gx", -1),
    ]
    up_half = (me < end) & ~(leg_out & odd)
    down_half = (me > 0) & ~(leg_out & (par == 0))
    low_half = (me > 0) & ~(leg_in & (par == 0))
    high_half = (me < end) & ~(leg_in & odd)

    def each(cond, copies, act):
        @pl.when(cond)
        def _():
            for c in copies:
                act(c)

    def go(c):
        c.start()

    hi_rows = slice(top, top + SUB)
    y_up = [
        copy(7, den.at[:, ny - SUB : ny], q.at[0, :, 0:SUB], "gy", 1),
        copy(8, mom.at[:, :, ny - SUB : ny], q.at[1:4, :, 0:SUB], "gy", 1),
        copy(9, en.at[:, ny - SUB : ny], q.at[4, :, 0:SUB], "gy", 1),
    ]
    y_down = [
        copy(10, den.at[:, 0:SUB], q.at[0, :, hi_rows], "gy", -1),
        copy(11, mom.at[:, :, 0:SUB], q.at[1:4, :, hi_rows], "gy", -1),
        copy(12, en.at[:, 0:SUB], q.at[4, :, hi_rows], "gy", -1),
        copy(13, disp.at[1, :, 0:SUB], dy.at[:, hi_rows], "gy", -1),
    ]
    z_up = [copy(14, edge, zlo, "gz", 1)]
    z_down = [copy(15, edge, zhi, "gz", -1)]

    def start(axis, ups, downs):
        @pl.when(pos[axis] < last[axis])
        def _():
            for c in ups:
                c.start()

        @pl.when(pos[axis] > 0)
        def _():
            for c in downs:
                c.start()

    def arrive(axis, ups, downs, fill_low, fill_high):
        @pl.when(pos[axis] > 0)
        def _():
            for c in ups:
                c.wait_recv()

        @pl.when(pos[axis] < last[axis])
        def _():
            for c in downs:
                c.wait_recv()

        @pl.when(pos[axis] == 0)
        def _():
            fill_low()

        @pl.when(pos[axis] == last[axis])
        def _():
            fill_high()

    def sent(axis, ups, downs):
        @pl.when(pos[axis] < last[axis])
        def _():
            for c in ups:
                c.wait_send()

        @pl.when(pos[axis] > 0)
        def _():
            for c in downs:
                c.wait_send()

    each(leg_out, legs, go)
    each(odd & (me < end), x_up, go)
    each(me > 0, x_down, go)
    each((par == 0) & (me < end), x_up, go)
    each(up_half, x_up_half, go)
    each(down_half, x_down_half, go)
    start("gy", y_up, y_down)

    for c in locals_:
        c.wait()

    flag = [flags[i].astype(jnp.float32) for i in range(6)]

    def low_mult(a):
        return jnp.where(pos[AXES[a]] == 0, flag[2 * a], 1.0)

    def high_mult(a):
        return jnp.where(pos[AXES[a]] == last[AXES[a]], flag[2 * a + 1], 1.0)

    def outer_low(a):
        return jnp.where(pos[AXES[a]] == 0, flag[2 * a], 0.0)

    def outer_high(a):
        return jnp.where(pos[AXES[a]] == last[AXES[a]], flag[2 * a + 1], 0.0)

    lane = lax.broadcasted_iota(jnp.int32, (ny, nz), 1)
    row = lax.broadcasted_iota(jnp.int32, (ny, nz), 0)

    def pack(x, carry):
        new = list(carry)
        for f in range(6):
            p = f * nx + x
            k = f * nx // per
            at = 4 * lax.rem(p, per)
            plane = q[f, x, SUB:top] if f < 5 else dz[x].astype(jnp.float32)
            moved = pltpu.roll(plane, at, 1)
            mine = lax.rem(lane + 2 - at + nz, nz) < 4
            new[k] = jnp.where(mine, moved, new[k])
        return tuple(new)

    packed = lax.fori_loop(0, nx, pack, tuple(jnp.zeros((ny, nz), jnp.float32) for _ in range(parts)))
    for k in range(parts):
        edge[k] = packed[k]

    wz = jnp.where(lane == 0, outer_low(2), 0.0) - jnp.where(lane == nz - 1, outer_high(2), 0.0)
    wy = jnp.where(row == 0, outer_low(1), 0.0) - jnp.where(row == ny - 1, outer_high(1), 0.0)
    wx_low, wx_high = outer_low(0), outer_high(0)

    def total(x, carry):
        a, b = carry
        wx = jnp.where(x == 0, wx_low, 0.0) - jnp.where(x == nx - 1, wx_high, 0.0)
        w = 1.0 + scale * (
            wz * dz[x].astype(jnp.float32)
            + wy * dy[x, SUB:top].astype(jnp.float32)
            + wx * dx[x].astype(jnp.float32)
        )
        return (
            a + jnp.sum((q[0, x, SUB:top] * w).reshape(ny // SUB, SUB, nz), 0),
            b + jnp.sum((q[4, x, SUB:top] * w).reshape(ny // SUB, SUB, nz), 0),
        )

    zero = jnp.zeros((SUB, nz), jnp.float32)
    mass, power = lax.fori_loop(0, nx, total, (zero, zero))
    sum_z[pos["gz"], 0] = mass
    sum_z[pos["gz"], 1] = power
    start("gz", z_up, z_down)

    def line(axis, slots, ss, rs):
        count = sizes[axis]
        copies = []
        for o in range(1, count):
            me = pos[axis]
            copies.append(
                pltpu.make_async_remote_copy(
                    src_ref=slots.at[me], dst_ref=slots.at[me], send_sem=ss.at[o],
                    recv_sem=rs.at[me], device_id={axis: lax.rem(me + o, count)},
                    device_id_type=pl.DeviceIdType.MESH,
                )
            )
        return copies

    def collect(axis, slots, ss, rs):
        count = sizes[axis]
        for o in range(1, count):
            peer = lax.rem(pos[axis] + o, count)
            pltpu.make_async_remote_copy(
                src_ref=slots.at[peer], dst_ref=slots.at[peer], send_sem=ss.at[o],
                recv_sem=rs.at[peer], device_id={axis: peer},
                device_id_type=pl.DeviceIdType.MESH,
            ).wait_recv()
        a, b = slots[0, 0], slots[0, 1]
        for o in range(1, count):
            a = a + slots[o, 0]
            b = b + slots[o, 1]
        return a, b

    line_z = line("gz", sum_z, ssz, rsz)
    line_y = line("gy", sum_y, ssy, rsy)
    line_x = line("gx", sum_x, ssx, rsx)
    for c in line_z:
        c.start()

    def z_low():
        e = edge[...]
        zlo[...] = jnp.where(lane3 & 3 == 3, pltpu.roll(e, nz - 1, 2), pltpu.roll(e, nz - 2, 2))

    def z_high():
        e = edge[...]
        zhi[...] = jnp.where(lane3 & 3 == 0, pltpu.roll(e, 1, 2), pltpu.roll(e, 2, 2))

    lane3 = lax.broadcasted_iota(jnp.int32, (parts, ny, nz), 2)
    arrive("gz", z_up, z_down, z_low, z_high)
    low = lane & 3 == 0
    for k in range(parts):
        e, l, h = edge[k], zlo[k], zhi[k]
        r1, r2 = pltpu.roll(l, 1, 1), pltpu.roll(l, 2, 1)
        l1, l2 = pltpu.roll(h, nz - 1, 1), pltpu.roll(h, nz - 2, 1)
        cq[k] = jnp.where(low, r1, l1)
        cs[k] = jnp.where(low, minmod(e - r1, r1 - r2), minmod(l2 - l1, l1 - e))

    first, final = lane == 0, lane == nz - 1
    z_lo_mult = jnp.where(first, low_mult(2), 1.0) * scale
    z_hi_mult = high_mult(2) * scale
    outs = (
        lambda x: out_d.at[x], lambda x: out_m.at[0, x], lambda x: out_m.at[1, x],
        lambda x: out_m.at[2, x], lambda x: out_e.at[x],
    )

    def along_z(x, _):
        v = dz[x].astype(jnp.float32) * z_lo_mult
        g = gain(v)

        def ghosts(ref, f):
            back = lax.rem(nz - 4 * lax.rem(f * nx + x, per), nz)
            return pltpu.roll(ref[f * nx // per], back, 1)

        vh = ghosts(cq, 5) * z_hi_mult
        gh = gain(vh)
        for f in range(5):
            plane = q[f, x, SUB:top]
            gq, gs = ghosts(cq, f), ghosts(cs, f)
            qm = jnp.where(first, gq, pltpu.roll(plane, 1, 1))
            d = plane - qm
            s = minmod(jnp.where(final, gq - plane, pltpu.roll(d, nz - 1, 1)), d)
            sm = jnp.where(first, gs, pltpu.roll(s, 1, 1))
            fl = flux(v, g, qm, plane, sm, s)
            fh = jnp.where(final, flux(vh, gh, plane, gq, s, gs), pltpu.roll(fl, nz - 1, 1))
            outs[f](x)[...] = plane + (fl - fh)
        return 0

    lax.fori_loop(0, nx, along_z, 0)

    @pl.when(relays)
    def _():
        for a, b in zip(legs, onward):
            a.wait_recv()
            b.start()

    a, b = collect("gz", sum_z, ssz, rsz)
    sum_y[pos["gy"], 0] = a
    sum_y[pos["gy"], 1] = b

    def y_low():
        q[:, :, 0:SUB] = jnp.broadcast_to(q[:, :, SUB : SUB + 1], (5, nx, SUB, nz))

    def y_high():
        q[:, :, hi_rows] = jnp.broadcast_to(q[:, :, top - 1 : top], (5, nx, SUB, nz))
        dy[:, hi_rows] = jnp.broadcast_to(dy[:, top - 1 : top], (nx, SUB, nz))

    arrive("gy", y_up, y_down, y_low, y_high)
    for c in line_y:
        c.start()
    tall = ny + 2 * SUB
    rows = lax.broadcasted_iota(jnp.int32, (tall, nz), 0)
    inside = (rows >= SUB) & (rows <= top)
    y_mult = jnp.where(
        rows == SUB, low_mult(1) * scale, jnp.where(rows == top, high_mult(1) * scale, scale)
    )

    def along_y(x, _):
        v = jnp.where(inside, dy[x].astype(jnp.float32), 0.0) * y_mult
        g = gain(v)
        for f in range(5):
            plane = q[f, x]
            qm = pltpu.roll(plane, 1, 0)
            d = plane - qm
            s = minmod(pltpu.roll(d, tall - 1, 0), d)
            fl = flux(v, g, qm, plane, pltpu.roll(s, 1, 0), s)
            ch = fl - pltpu.roll(fl, tall - 1, 0)
            outs[f](x)[...] += ch[SUB:top]
        return 0

    lax.fori_loop(0, nx, along_y, 0)

    a, b = collect("gy", sum_y, ssy, rsy)
    sum_x[pos["gx"], 0] = a
    sum_x[pos["gx"], 1] = b

    def core(r, _):
        at = pl.ds(pl.multiple_of(r * SUB, SUB), SUB)
        inner = pl.ds(pl.multiple_of(r * SUB + SUB, SUB), SUB)
        vs = [dx[c, at].astype(jnp.float32) * scale for c in range(2, nx - 1)]
        gs = [gain(v) for v in vs]
        for f in range(5):
            line_q = [q[f, c, inner] for c in range(nx)]
            ds = [line_q[i + 1] - line_q[i] for i in range(nx - 1)]
            ss = [minmod(ds[i + 1], ds[i]) for i in range(nx - 2)]
            fl = [
                flux(vs[i], gs[i], line_q[i + 1], line_q[i + 2], ss[i], ss[i + 1])
                for i in range(nx - 3)
            ]
            for c in range(1, nx - 1):
                change = fl[c - 2] if c >= 2 else 0.0
                ref = outs[f](c)
                ref[at] += change - fl[c - 1] if c < nx - 2 else change
        return 0

    lax.fori_loop(0, ny // SUB, core, 0)

    def x_low():
        xlo[...] = jnp.broadcast_to(q[:, 0:1, SUB:top], (5, 2, ny, nz))

    def x_high():
        xhi[...] = jnp.broadcast_to(q[:, nx - 1 : nx, SUB:top], (5, 2, ny, nz))
        xv[...] = dx[nx - 1]

    for c in line_x:
        c.start()
    each(low_half, x_up_half, lambda c: c.wait_recv())
    each(high_half, x_down_half, lambda c: c.wait_recv())
    each(leg_in, landed, lambda c: c.wait_recv())
    arrive("gx", x_up, x_down, x_low, x_high)
    x_lo_mult, x_hi_mult = low_mult(0) * scale, high_mult(0) * scale

    def x_rows(r):
        return pl.ds(pl.multiple_of(r * SUB, SUB), SUB), pl.ds(
            pl.multiple_of(r * SUB + SUB, SUB), SUB
        )

    def x_flux(v, g, cells4):
        ds = [cells4[i + 1] - cells4[i] for i in range(3)]
        return flux(
            v, g, cells4[1], cells4[2], minmod(ds[1], ds[0]), minmod(ds[2], ds[1])
        )

    def rim(r, _):
        at, inner = x_rows(r)
        faces = (0, 1, nx - 1, nx)
        vs = [
            dx[0, at].astype(jnp.float32) * x_lo_mult,
            dx[1, at].astype(jnp.float32) * scale,
            dx[nx - 1, at].astype(jnp.float32) * scale,
            xv[at].astype(jnp.float32) * x_hi_mult,
        ]
        gs = [gain(v) for v in vs]
        for f in range(5):
            a = [xlo[f, 0, at], xlo[f, 1, at]] + [q[f, c, inner] for c in range(3)]
            b = [q[f, c, inner] for c in range(nx - 3, nx)] + [xhi[f, 0, at], xhi[f, 1, at]]
            fl = [x_flux(vs[i], gs[i], (a, a, b, b)[i][i % 2 : i % 2 + 4]) for i in range(4)]
            for c, change in (
                (0, fl[0] - fl[1]), (1, fl[1]), (nx - 2, -fl[2]), (nx - 1, fl[2] - fl[3]),
            ):
                ref = outs[f](c)
                ref[at] += change
        return 0

    lax.fori_loop(0, ny // SUB, rim, 0)

    a, b = collect("gx", sum_x, ssx, rsx)
    sums[0] = a
    sums[1] = b
    sent("gx", x_up, x_down)
    each(leg_out, legs, lambda c: c.wait_send())
    each(relays, onward, lambda c: c.wait_send())
    each(up_half, x_up_half, lambda c: c.wait_send())
    each(down_half, x_down_half, lambda c: c.wait_send())
    sent("gy", y_up, y_down)
    sent("gz", z_up, z_down)
    for c in line_x + line_y + line_z:
        c.wait_send()


def put(cells, den, mom, en, sums, out_d, out_m, out_e, totals, sem):
    moves = [
        pltpu.make_async_copy(src, dst, sem.at[i])
        for i, (src, dst) in enumerate(((mom, out_m), (den, out_d), (en, out_e)))
    ]
    for c in moves:
        c.start()
    totals[0] = jnp.sum(sums[0]) / cells
    totals[1] = jnp.sum(sums[1]) / cells
    for c in moves:
        c.wait()


def shards(density, momentum, energy, displacement, flags):
    sizes = {a: lax.axis_size(a) for a in AXES}
    nx, ny, nz = density.shape
    tall = ny + 2 * SUB
    per = nz // 4
    parts = -(-6 * nx // per)
    f32, i32 = jnp.float32, jnp.int32
    dma = pltpu.SemaphoreType.DMA
    any_ = pl.BlockSpec(memory_space=pl.ANY)
    hbm = pl.BlockSpec(memory_space=pltpu.HBM)
    vmem = pl.BlockSpec(memory_space=pltpu.VMEM)
    smem = pl.BlockSpec(memory_space=pltpu.SMEM)
    cells = float(nx * ny * nz)
    for a in AXES:
        cells = cells * sizes[a]
    outputs = tuple(jax.ShapeDtypeStruct(v.shape, f32) for v in (density, momentum, energy))
    results = pl.pallas_call(
        functools.partial(kernel, sizes),
        out_shape=outputs + (jax.ShapeDtypeStruct((2, SUB, nz), f32),),
        in_specs=[hbm] * 5,
        out_specs=(vmem, vmem, vmem, vmem),
        scratch_shapes=[
            pltpu.SMEM((6,), i32),
            pltpu.VMEM((5, nx, tall, nz), f32),
            pltpu.VMEM((nx, ny, nz), i32),
            pltpu.VMEM((nx, tall, nz), i32),
            pltpu.VMEM((nx, ny, nz), i32),
            pltpu.VMEM((2, 5, 2, ny, nz), f32),
            pltpu.VMEM((5, ny, nz), f32),
            pltpu.VMEM((ny, nz), i32),
        ]
        + [pltpu.VMEM((parts, ny, nz), f32) for _ in range(5)]
        + [pltpu.VMEM((sizes[a], 2, SUB, nz), f32) for a in AXES]
        + [dma((7,)), dma((26,)), dma((26,))]
        + [dma((sizes[a],)) for a in AXES for _ in range(2)],
        compiler_params=pltpu.CompilerParams(
            collective_id=0, has_side_effects=True, vmem_limit_bytes=12 << 20
        ),
    )(
        *(
            pltpu.with_memory_space_constraint(v, pltpu.HBM)
            for v in (flags, density, momentum, energy, displacement)
        )
    )
    return pl.pallas_call(
        functools.partial(put, cells),
        out_shape=outputs + (jax.ShapeDtypeStruct((2,), f32),),
        in_specs=[any_, any_, any_, vmem],
        out_specs=(hbm, hbm, hbm, smem),
        scratch_shapes=[dma((3,))],
        compiler_params=pltpu.CompilerParams(vmem_limit_bytes=2 << 20),
    )(*results)


def solution(mesh):
    return jax.shard_map(
        shards,
        mesh=mesh,
        in_specs=(
            P("gx", "gy", "gz"),
            P(None, "gx", "gy", "gz"),
            P("gx", "gy", "gz"),
            P(None, "gx", "gy", "gz"),
            P(),
        ),
        out_specs=(P("gx", "gy", "gz"), P(None, "gx", "gy", "gz"), P("gx", "gy", "gz"), P()),
        check_vma=False,
    )
```

```python
import functools

import jax
import jax.numpy as jnp
from jax import lax
from jax.experimental import pallas as pl
from jax.experimental.pallas import tpu as pltpu
from jax.sharding import PartitionSpec as P

AXES = ("gx", "gy", "gz")
SUB = 8


def minmod(p, r):
    return jnp.maximum(jnp.minimum(r, 0.0), jnp.minimum(p, jnp.maximum(r, 0.0)))


def gain(v):
    size = jnp.abs(v)
    return 0.5 * size * (1.0 - size)


def flux(v, g, q_low, q_high, s_low, s_high):
    up = v > 0
    return v * jnp.where(up, q_low, q_high) + g * jnp.where(up, s_low, s_high)


def kernel(
    sizes, flags_in, den, mom, en, disp, out_d, out_m, out_e, sums,
    flags, q, dx, dy, dz, xh, hop, xv, edge, zlo, zhi, cq, cs, sum_x, sum_y, sum_z,
    local_sem, send_sem, recv_sem, ssx, rsx, ssy, rsy, ssz, rsz,
):
    nx, ny, nz = den.shape
    pos = {a: lax.axis_index(a) for a in AXES}
    top = ny + SUB
    per = nz // 4
    parts = edge.shape[0]
    scale = 1.0 / 256.0
    xlo, xhi = xh.at[0], xh.at[1]

    barrier = pltpu.get_barrier_semaphore()
    greeted = 0
    for a in ("gy", "gx", "gz"):
        for o in range(1, sizes[a]):
            peer = lax.rem(pos[a] + o, sizes[a])
            pl.semaphore_signal(
                barrier, inc=1, device_id={a: peer}, device_id_type=pl.DeviceIdType.MESH
            )
            greeted += 1

    locals_ = [
        pltpu.make_async_copy(den, q.at[0, :, SUB:top], local_sem.at[0]),
        pltpu.make_async_copy(mom, q.at[1:4, :, SUB:top], local_sem.at[1]),
        pltpu.make_async_copy(en, q.at[4, :, SUB:top], local_sem.at[2]),
        pltpu.make_async_copy(disp.at[2], dz, local_sem.at[3]),
        pltpu.make_async_copy(disp.at[1], dy.at[:, SUB:top], local_sem.at[4]),
        pltpu.make_async_copy(disp.at[0], dx, local_sem.at[5]),
        pltpu.make_async_copy(flags_in, flags, local_sem.at[6]),
    ]
    for c in locals_:
        c.start()

    pl.semaphore_wait(barrier, greeted)

    def copy(k, src, dst, axis, step):
        return pltpu.make_async_remote_copy(
            src_ref=src, dst_ref=dst, send_sem=send_sem.at[k], recv_sem=recv_sem.at[k],
            device_id={axis: pos[axis] + step}, device_id_type=pl.DeviceIdType.MESH,
        )

    last = {a: sizes[a] - 1 for a in AXES}
    me = pos["gx"]
    par = lax.rem(me, 2)
    odd = par == 1
    end = last["gx"]
    leg_out = (odd & (me + 2 <= end)) | ((par == 0) & (me >= 2))
    relays = (odd & (me >= 3)) | ((par == 0) & (me + 2 <= end))
    leg_in = (me + 1 <= end) & (odd | (me >= 2))
    begin = par * (nx - 2)
    other = 1 - par

    def remote(k, src, dst, target):
        return pltpu.make_async_remote_copy(
            src_ref=src, dst_ref=dst, send_sem=send_sem.at[k], recv_sem=recv_sem.at[k],
            device_id={"gx": target}, device_id_type=pl.DeviceIdType.MESH,
        )

    over = me + 4 * par - 2
    legs = [
        remote(16, mom.at[0, pl.ds(begin, 2)], hop.at[0:2], over),
        remote(17, mom.at[1, pl.ds(begin, 2)], hop.at[2:4], over),
        remote(18, en.at[begin], hop.at[4], over),
    ]
    beside = me + 1 - 2 * par
    onward = [
        remote(19, hop.at[0:2], xh.at[other, 1], beside),
        remote(20, hop.at[2:4], xh.at[other, 2], beside),
        remote(21, hop.at[4], xh.at[other, 4, 0], beside),
    ]
    landed = [
        remote(19, hop.at[0:2], xh.at[par, 1], beside),
        remote(20, hop.at[2:4], xh.at[par, 2], beside),
        remote(21, hop.at[4], xh.at[par, 4, 0], beside),
    ]
    x_up = [
        copy(0, den.at[nx - 2 : nx], xlo.at[0], "gx", 1),
        copy(1, mom.at[2, nx - 2 : nx], xlo.at[3], "gx", 1),
        copy(2, en.at[nx - 1], xlo.at[4, 1], "gx", 1),
    ]
    x_up_half = [
        copy(22, mom.at[0:2, nx - 2 : nx], xlo.at[1:3], "gx", 1),
        copy(23, en.at[nx - 2], xlo.at[4, 0], "gx", 1),
    ]
    x_down = [
        copy(6, disp.at[0, 0], xv, "gx", -1),
        copy(3, den.at[0:2], xhi.at[0], "gx", -1),
        copy(4, mom.at[2, 0:2], xhi.at[3], "gx", -1),
        copy(5, en.at[1], xhi.at[4, 1], "gx", -1),
    ]
    x_down_half = [
        copy(24, mom.at[0:2, 0:2], xhi.at[1:3], "gx", -1),
        copy(25, en.at[0], xhi.at[4, 0], "gx", -1),
    ]
    up_half = (me < end) & ~(leg_out & odd)
    down_half = (me > 0) & ~(leg_out & (par == 0))
    low_half = (me > 0) & ~(leg_in & (par == 0))
    high_half = (me < end) & ~(leg_in & odd)

    def each(cond, copies, act):
        @pl.when(cond)
        def _():
            for c in copies:
                act(c)

    def go(c):
        c.start()

    hi_rows = slice(top, top + SUB)
    y_up = [
        copy(7, den.at[:, ny - SUB : ny], q.at[0, :, 0:SUB], "gy", 1),
        copy(8, mom.at[:, :, ny - SUB : ny], q.at[1:4, :, 0:SUB], "gy", 1),
        copy(9, en.at[:, ny - SUB : ny], q.at[4, :, 0:SUB], "gy", 1),
    ]
    y_down = [
        copy(10, den.at[:, 0:SUB], q.at[0, :, hi_rows], "gy", -1),
        copy(11, mom.at[:, :, 0:SUB], q.at[1:4, :, hi_rows], "gy", -1),
        copy(12, en.at[:, 0:SUB], q.at[4, :, hi_rows], "gy", -1),
        copy(13, disp.at[1, :, 0:SUB], dy.at[:, hi_rows], "gy", -1),
    ]
    z_up = [copy(14, edge, zlo, "gz", 1)]
    z_down = [copy(15, edge, zhi, "gz", -1)]

    def start(axis, ups, downs):
        @pl.when(pos[axis] < last[axis])
        def _():
            for c in ups:
                c.start()

        @pl.when(pos[axis] > 0)
        def _():
            for c in downs:
                c.start()

    def arrive(axis, ups, downs, fill_low, fill_high):
        @pl.when(pos[axis] > 0)
        def _():
            for c in ups:
                c.wait_recv()

        @pl.when(pos[axis] < last[axis])
        def _():
            for c in downs:
                c.wait_recv()

        @pl.when(pos[axis] == 0)
        def _():
            fill_low()

        @pl.when(pos[axis] == last[axis])
        def _():
            fill_high()

    def sent(axis, ups, downs):
        @pl.when(pos[axis] < last[axis])
        def _():
            for c in ups:
                c.wait_send()

        @pl.when(pos[axis] > 0)
        def _():
            for c in downs:
                c.wait_send()

    each(leg_out, legs, go)
    each(odd & (me < end), x_up, go)
    each(me > 0, x_down, go)
    each((par == 0) & (me < end), x_up, go)
    each(up_half, x_up_half, go)
    each(down_half, x_down_half, go)
    start("gy", y_up, y_down)

    for c in locals_:
        c.wait()

    flag = [flags[i].astype(jnp.float32) for i in range(6)]

    def low_mult(a):
        return jnp.where(pos[AXES[a]] == 0, flag[2 * a], 1.0)

    def high_mult(a):
        return jnp.where(pos[AXES[a]] == last[AXES[a]], flag[2 * a + 1], 1.0)

    def outer_low(a):
        return jnp.where(pos[AXES[a]] == 0, flag[2 * a], 0.0)

    def outer_high(a):
        return jnp.where(pos[AXES[a]] == last[AXES[a]], flag[2 * a + 1], 0.0)

    lane = lax.broadcasted_iota(jnp.int32, (ny, nz), 1)
    row = lax.broadcasted_iota(jnp.int32, (ny, nz), 0)

    def pack(x, carry):
        new = list(carry)
        for f in range(6):
            p = f * nx + x
            k = f * nx // per
            at = 4 * lax.rem(p, per)
            plane = q[f, x, SUB:top] if f < 5 else dz[x].astype(jnp.float32)
            moved = pltpu.roll(plane, at, 1)
            mine = lax.rem(lane + 2 - at + nz, nz) < 4
            new[k] = jnp.where(mine, moved, new[k])
        return tuple(new)

    packed = lax.fori_loop(0, nx, pack, tuple(jnp.zeros((ny, nz), jnp.float32) for _ in range(parts)))
    for k in range(parts):
        edge[k] = packed[k]

    wz = jnp.where(lane == 0, outer_low(2), 0.0) - jnp.where(lane == nz - 1, outer_high(2), 0.0)
    wy = jnp.where(row == 0, outer_low(1), 0.0) - jnp.where(row == ny - 1, outer_high(1), 0.0)
    wx_low, wx_high = outer_low(0), outer_high(0)

    def total(x, carry):
        a, b = carry
        wx = jnp.where(x == 0, wx_low, 0.0) - jnp.where(x == nx - 1, wx_high, 0.0)
        w = 1.0 + scale * (
            wz * dz[x].astype(jnp.float32)
            + wy * dy[x, SUB:top].astype(jnp.float32)
            + wx * dx[x].astype(jnp.float32)
        )
        return (
            a + jnp.sum((q[0, x, SUB:top] * w).reshape(ny // SUB, SUB, nz), 0),
            b + jnp.sum((q[4, x, SUB:top] * w).reshape(ny // SUB, SUB, nz), 0),
        )

    zero = jnp.zeros((SUB, nz), jnp.float32)
    mass, power = lax.fori_loop(0, nx, total, (zero, zero))
    sum_z[pos["gz"], 0] = mass
    sum_z[pos["gz"], 1] = power
    start("gz", z_up, z_down)

    def line(axis, slots, ss, rs):
        count = sizes[axis]
        copies = []
        for o in range(1, count):
            me = pos[axis]
            copies.append(
                pltpu.make_async_remote_copy(
                    src_ref=slots.at[me], dst_ref=slots.at[me], send_sem=ss.at[o],
                    recv_sem=rs.at[me], device_id={axis: lax.rem(me + o, count)},
                    device_id_type=pl.DeviceIdType.MESH,
                )
            )
        return copies

    def collect(axis, slots, ss, rs):
        count = sizes[axis]
        for o in range(1, count):
            peer = lax.rem(pos[axis] + o, count)
            pltpu.make_async_remote_copy(
                src_ref=slots.at[peer], dst_ref=slots.at[peer], send_sem=ss.at[o],
                recv_sem=rs.at[peer], device_id={axis: peer},
                device_id_type=pl.DeviceIdType.MESH,
            ).wait_recv()
        a, b = slots[0, 0], slots[0, 1]
        for o in range(1, count):
            a = a + slots[o, 0]
            b = b + slots[o, 1]
        return a, b

    line_z = line("gz", sum_z, ssz, rsz)
    line_y = line("gy", sum_y, ssy, rsy)
    line_x = line("gx", sum_x, ssx, rsx)
    for c in line_z:
        c.start()

    def z_low():
        e = edge[...]
        zlo[...] = jnp.where(lane3 & 3 == 3, pltpu.roll(e, nz - 1, 2), pltpu.roll(e, nz - 2, 2))

    def z_high():
        e = edge[...]
        zhi[...] = jnp.where(lane3 & 3 == 0, pltpu.roll(e, 1, 2), pltpu.roll(e, 2, 2))

    lane3 = lax.broadcasted_iota(jnp.int32, (parts, ny, nz), 2)
    arrive("gz", z_up, z_down, z_low, z_high)
    low = lane & 3 == 0
    for k in range(parts):
        e, l, h = edge[k], zlo[k], zhi[k]
        r1, r2 = pltpu.roll(l, 1, 1), pltpu.roll(l, 2, 1)
        l1, l2 = pltpu.roll(h, nz - 1, 1), pltpu.roll(h, nz - 2, 1)
        cq[k] = jnp.where(low, r1, l1)
        cs[k] = jnp.where(low, minmod(e - r1, r1 - r2), minmod(l2 - l1, l1 - e))

    first, final = lane == 0, lane == nz - 1
    z_lo_mult = jnp.where(first, low_mult(2), 1.0) * scale
    z_hi_mult = high_mult(2) * scale
    outs = (
        lambda x: out_d.at[x], lambda x: out_m.at[0, x], lambda x: out_m.at[1, x],
        lambda x: out_m.at[2, x], lambda x: out_e.at[x],
    )

    def along_z(x, _):
        v = dz[x].astype(jnp.float32) * z_lo_mult
        g = gain(v)

        def ghosts(ref, f):
            back = lax.rem(nz - 4 * lax.rem(f * nx + x, per), nz)
            return pltpu.roll(ref[f * nx // per], back, 1)

        vh = ghosts(cq, 5) * z_hi_mult
        gh = gain(vh)
        for f in range(5):
            plane = q[f, x, SUB:top]
            gq, gs = ghosts(cq, f), ghosts(cs, f)
            qm = jnp.where(first, gq, pltpu.roll(plane, 1, 1))
            d = plane - qm
            s = minmod(jnp.where(final, gq - plane, pltpu.roll(d, nz - 1, 1)), d)
            sm = jnp.where(first, gs, pltpu.roll(s, 1, 1))
            fl = flux(v, g, qm, plane, sm, s)
            fh = jnp.where(final, flux(vh, gh, plane, gq, s, gs), pltpu.roll(fl, nz - 1, 1))
            outs[f](x)[...] = plane + (fl - fh)
        return 0

    lax.fori_loop(0, nx, along_z, 0)

    @pl.when(relays)
    def _():
        for a, b in zip(legs, onward):
            a.wait_recv()
            b.start()

    a, b = collect("gz", sum_z, ssz, rsz)
    sum_y[pos["gy"], 0] = a
    sum_y[pos["gy"], 1] = b

    def y_low():
        q[:, :, 0:SUB] = jnp.broadcast_to(q[:, :, SUB : SUB + 1], (5, nx, SUB, nz))

    def y_high():
        q[:, :, hi_rows] = jnp.broadcast_to(q[:, :, top - 1 : top], (5, nx, SUB, nz))
        dy[:, hi_rows] = jnp.broadcast_to(dy[:, top - 1 : top], (nx, SUB, nz))

    arrive("gy", y_up, y_down, y_low, y_high)
    for c in line_y:
        c.start()
    tall = ny + 2 * SUB
    rows = lax.broadcasted_iota(jnp.int32, (tall, nz), 0)
    inside = (rows >= SUB) & (rows <= top)
    y_mult = jnp.where(
        rows == SUB, low_mult(1) * scale, jnp.where(rows == top, high_mult(1) * scale, scale)
    )

    def along_y(x, _):
        v = jnp.where(inside, dy[x].astype(jnp.float32), 0.0) * y_mult
        g = gain(v)
        for f in range(5):
            plane = q[f, x]
            qm = pltpu.roll(plane, 1, 0)
            d = plane - qm
            s = minmod(pltpu.roll(d, tall - 1, 0), d)
            fl = flux(v, g, qm, plane, pltpu.roll(s, 1, 0), s)
            ch = fl - pltpu.roll(fl, tall - 1, 0)
            outs[f](x)[...] += ch[SUB:top]
        return 0

    lax.fori_loop(0, nx, along_y, 0)

    a, b = collect("gy", sum_y, ssy, rsy)
    sum_x[pos["gx"], 0] = a
    sum_x[pos["gx"], 1] = b

    def core(r, _):
        at = pl.ds(pl.multiple_of(r * SUB, SUB), SUB)
        inner = pl.ds(pl.multiple_of(r * SUB + SUB, SUB), SUB)
        vs = [dx[c, at].astype(jnp.float32) * scale for c in range(2, nx - 1)]
        gs = [gain(v) for v in vs]
        for f in range(5):
            line_q = [q[f, c, inner] for c in range(nx)]
            ds = [line_q[i + 1] - line_q[i] for i in range(nx - 1)]
            ss = [minmod(ds[i + 1], ds[i]) for i in range(nx - 2)]
            fl = [
                flux(vs[i], gs[i], line_q[i + 1], line_q[i + 2], ss[i], ss[i + 1])
                for i in range(nx - 3)
            ]
            for c in range(1, nx - 1):
                change = fl[c - 2] if c >= 2 else 0.0
                ref = outs[f](c)
                ref[at] += change - fl[c - 1] if c < nx - 2 else change
        return 0

    lax.fori_loop(0, ny // SUB, core, 0)

    def x_low():
        xlo[...] = jnp.broadcast_to(q[:, 0:1, SUB:top], (5, 2, ny, nz))

    def x_high():
        xhi[...] = jnp.broadcast_to(q[:, nx - 1 : nx, SUB:top], (5, 2, ny, nz))
        xv[...] = dx[nx - 1]

    for c in line_x:
        c.start()
    arrive("gx", x_up, x_down, x_low, x_high)
    x_lo_mult, x_hi_mult = low_mult(0) * scale, high_mult(0) * scale

    def x_rows(r):
        return pl.ds(pl.multiple_of(r * SUB, SUB), SUB), pl.ds(
            pl.multiple_of(r * SUB + SUB, SUB), SUB
        )

    def x_flux(v, g, cells4):
        ds = [cells4[i + 1] - cells4[i] for i in range(3)]
        return flux(
            v, g, cells4[1], cells4[2], minmod(ds[1], ds[0]), minmod(ds[2], ds[1])
        )

    def rim(fields, r, _):
        at, inner = x_rows(r)
        faces = (0, 1, nx - 1, nx)
        vs = [
            dx[0, at].astype(jnp.float32) * x_lo_mult,
            dx[1, at].astype(jnp.float32) * scale,
            dx[nx - 1, at].astype(jnp.float32) * scale,
            xv[at].astype(jnp.float32) * x_hi_mult,
        ]
        gs = [gain(v) for v in vs]
        for f in fields:
            a = [xlo[f, 0, at], xlo[f, 1, at]] + [q[f, c, inner] for c in range(3)]
            b = [q[f, c, inner] for c in range(nx - 3, nx)] + [xhi[f, 0, at], xhi[f, 1, at]]
            fl = [x_flux(vs[i], gs[i], (a, a, b, b)[i][i % 2 : i % 2 + 4]) for i in range(4)]
            for c, change in (
                (0, fl[0] - fl[1]), (1, fl[1]), (nx - 2, -fl[2]), (nx - 1, fl[2] - fl[3]),
            ):
                ref = outs[f](c)
                ref[at] += change
        return 0

    lax.fori_loop(0, ny // SUB, functools.partial(rim, (0, 3)), 0)
    each(low_half, x_up_half, lambda c: c.wait_recv())
    each(high_half, x_down_half, lambda c: c.wait_recv())
    each(leg_in, landed, lambda c: c.wait_recv())
    lax.fori_loop(0, ny // SUB, functools.partial(rim, (1, 2, 4)), 0)

    a, b = collect("gx", sum_x, ssx, rsx)
    sums[0] = a
    sums[1] = b
    sent("gx", x_up, x_down)
    each(leg_out, legs, lambda c: c.wait_send())
    each(relays, onward, lambda c: c.wait_send())
    each(up_half, x_up_half, lambda c: c.wait_send())
    each(down_half, x_down_half, lambda c: c.wait_send())
    sent("gy", y_up, y_down)
    sent("gz", z_up, z_down)
    for c in line_x + line_y + line_z:
        c.wait_send()


def put(cells, den, mom, en, sums, out_d, out_m, out_e, totals, sem):
    pairs = [(den, out_d), (en, out_e)] + [(mom.at[c], out_m.at[c]) for c in range(3)]
    half = den.shape[0] // 2
    pairs = [
        (src.at[at], dst.at[at])
        for src, dst in pairs
        for at in (slice(0, half), slice(half, 2 * half))
    ]
    moves = [
        pltpu.make_async_copy(src, dst, sem.at[i]) for i, (src, dst) in enumerate(pairs)
    ]
    for c in moves:
        c.start()
    totals[0] = jnp.sum(sums[0]) / cells
    totals[1] = jnp.sum(sums[1]) / cells
    for c in moves:
        c.wait()


def shards(density, momentum, energy, displacement, flags):
    sizes = {a: lax.axis_size(a) for a in AXES}
    nx, ny, nz = density.shape
    tall = ny + 2 * SUB
    per = nz // 4
    parts = -(-6 * nx // per)
    f32, i32 = jnp.float32, jnp.int32
    dma = pltpu.SemaphoreType.DMA
    any_ = pl.BlockSpec(memory_space=pl.ANY)
    hbm = pl.BlockSpec(memory_space=pltpu.HBM)
    vmem = pl.BlockSpec(memory_space=pltpu.VMEM)
    smem = pl.BlockSpec(memory_space=pltpu.SMEM)
    cells = float(nx * ny * nz)
    for a in AXES:
        cells = cells * sizes[a]
    outputs = tuple(jax.ShapeDtypeStruct(v.shape, f32) for v in (density, momentum, energy))
    results = pl.pallas_call(
        functools.partial(kernel, sizes),
        out_shape=outputs + (jax.ShapeDtypeStruct((2, SUB, nz), f32),),
        in_specs=[hbm] * 5,
        out_specs=(vmem, vmem, vmem, vmem),
        scratch_shapes=[
            pltpu.SMEM((6,), i32),
            pltpu.VMEM((5, nx, tall, nz), f32),
            pltpu.VMEM((nx, ny, nz), i32),
            pltpu.VMEM((nx, tall, nz), i32),
            pltpu.VMEM((nx, ny, nz), i32),
            pltpu.VMEM((2, 5, 2, ny, nz), f32),
            pltpu.VMEM((5, ny, nz), f32),
            pltpu.VMEM((ny, nz), i32),
        ]
        + [pltpu.VMEM((parts, ny, nz), f32) for _ in range(5)]
        + [pltpu.VMEM((sizes[a], 2, SUB, nz), f32) for a in AXES]
        + [dma((7,)), dma((26,)), dma((26,))]
        + [dma((sizes[a],)) for a in AXES for _ in range(2)],
        compiler_params=pltpu.CompilerParams(
            collective_id=0, has_side_effects=True, vmem_limit_bytes=12 << 20
        ),
    )(
        *(
            pltpu.with_memory_space_constraint(v, pltpu.HBM)
            for v in (flags, density, momentum, energy, displacement)
        )
    )
    return pl.pallas_call(
        functools.partial(put, cells),
        out_shape=outputs + (jax.ShapeDtypeStruct((2,), f32),),
        in_specs=[any_, any_, any_, vmem],
        out_specs=(hbm, hbm, hbm, smem),
        scratch_shapes=[dma((10,))],
        compiler_params=pltpu.CompilerParams(vmem_limit_bytes=2 << 20),
    )(*results)


def solution(mesh):
    return jax.shard_map(
        shards,
        mesh=mesh,
        in_specs=(
            P("gx", "gy", "gz"),
            P(None, "gx", "gy", "gz"),
            P("gx", "gy", "gz"),
            P(None, "gx", "gy", "gz"),
            P(),
        ),
        out_specs=(P("gx", "gy", "gz"), P(None, "gx", "gy", "gz"), P("gx", "gy", "gz"), P()),
        check_vma=False,
    )
```

```python
import functools

import jax
import jax.numpy as jnp
from jax import lax
from jax.experimental import pallas as pl
from jax.experimental.pallas import tpu as pltpu
from jax.sharding import PartitionSpec as P

AXES = ("gx", "gy", "gz")
SUB = 8


def minmod(p, r):
    return jnp.maximum(jnp.minimum(r, 0.0), jnp.minimum(p, jnp.maximum(r, 0.0)))


def gain(v):
    size = jnp.abs(v)
    return 0.5 * size * (1.0 - size)


def flux(v, g, q_low, q_high, s_low, s_high):
    up = v > 0
    return v * jnp.where(up, q_low, q_high) + g * jnp.where(up, s_low, s_high)


def kernel(
    sizes, flags_in, den, mom, en, disp, out_d, out_m, out_e, sums,
    flags, q, dx, dy, dz, xh, hop, xv, edge, zlo, zhi, cq, cs, sum_x, sum_y, sum_z,
    local_sem, send_sem, recv_sem, ssx, rsx, ssy, rsy, ssz, rsz,
):
    nx, ny, nz = den.shape
    pos = {a: lax.axis_index(a) for a in AXES}
    top = ny + SUB
    per = nz // 4
    parts = edge.shape[0]
    scale = 1.0 / 256.0
    xlo, xhi = xh.at[0], xh.at[1]

    barrier = pltpu.get_barrier_semaphore()
    doubling = sizes["gy"] & (sizes["gy"] - 1) == 0
    strides = [1 << i for i in range(sizes["gy"].bit_length() - 1)] if doubling else []

    def across(stride):
        return pos["gy"] + stride - 2 * stride * lax.rem(pos["gy"] // stride, 2)

    def greet(axis, peer):
        pl.semaphore_signal(
            barrier, inc=1, device_id={axis: peer}, device_id_type=pl.DeviceIdType.MESH
        )

    greeted = 0
    for a in ("gx", "gy", "gz"):
        if a == "gy" and doubling:
            for stride in strides:
                greet(a, across(stride))
                greeted += 1
            for step in (1, -1):
                @pl.when((pos[a] + step >= 0) & (pos[a] + step < sizes[a]))
                def _():
                    greet(a, pos[a] + step)

            greeted += jnp.where(pos[a] > 0, 1, 0) + jnp.where(pos[a] < sizes[a] - 1, 1, 0)
        else:
            for o in range(1, sizes[a]):
                greet(a, lax.rem(pos[a] + o, sizes[a]))
                greeted += 1

    locals_ = [
        pltpu.make_async_copy(den, q.at[0, :, SUB:top], local_sem.at[0]),
        pltpu.make_async_copy(mom, q.at[1:4, :, SUB:top], local_sem.at[1]),
        pltpu.make_async_copy(en, q.at[4, :, SUB:top], local_sem.at[2]),
        pltpu.make_async_copy(disp.at[2], dz, local_sem.at[3]),
        pltpu.make_async_copy(disp.at[1], dy.at[:, SUB:top], local_sem.at[4]),
        pltpu.make_async_copy(disp.at[0], dx, local_sem.at[5]),
        pltpu.make_async_copy(flags_in, flags, local_sem.at[6]),
    ]
    for c in locals_:
        c.start()

    pl.semaphore_wait(barrier, greeted)

    def copy(k, src, dst, axis, step):
        return pltpu.make_async_remote_copy(
            src_ref=src, dst_ref=dst, send_sem=send_sem.at[k], recv_sem=recv_sem.at[k],
            device_id={axis: pos[axis] + step}, device_id_type=pl.DeviceIdType.MESH,
        )

    last = {a: sizes[a] - 1 for a in AXES}
    me = pos["gx"]
    par = lax.rem(me, 2)
    odd = par == 1
    end = last["gx"]
    leg_out = (odd & (me + 2 <= end)) | ((par == 0) & (me >= 2))
    relays = (odd & (me >= 3)) | ((par == 0) & (me + 2 <= end))
    leg_in = (me + 1 <= end) & (odd | (me >= 2))
    begin = par * (nx - 2)
    other = 1 - par

    def remote(k, src, dst, target):
        return pltpu.make_async_remote_copy(
            src_ref=src, dst_ref=dst, send_sem=send_sem.at[k], recv_sem=recv_sem.at[k],
            device_id={"gx": target}, device_id_type=pl.DeviceIdType.MESH,
        )

    over = me + 4 * par - 2
    legs = [
        remote(16, mom.at[0, pl.ds(begin, 2)], hop.at[0:2], over),
        remote(17, mom.at[1, pl.ds(begin, 2)], hop.at[2:4], over),
        remote(18, en.at[begin], hop.at[4], over),
    ]
    beside = me + 1 - 2 * par
    onward = [
        remote(19, hop.at[0:2], xh.at[other, 1], beside),
        remote(20, hop.at[2:4], xh.at[other, 2], beside),
        remote(21, hop.at[4], xh.at[other, 4, 0], beside),
    ]
    landed = [
        remote(19, hop.at[0:2], xh.at[par, 1], beside),
        remote(20, hop.at[2:4], xh.at[par, 2], beside),
        remote(21, hop.at[4], xh.at[par, 4, 0], beside),
    ]
    x_up = [
        copy(0, den.at[nx - 2 : nx], xlo.at[0], "gx", 1),
        copy(1, mom.at[2, nx - 2 : nx], xlo.at[3], "gx", 1),
        copy(2, en.at[nx - 1], xlo.at[4, 1], "gx", 1),
    ]
    x_up_half = [
        copy(22, mom.at[0:2, nx - 2 : nx], xlo.at[1:3], "gx", 1),
        copy(23, en.at[nx - 2], xlo.at[4, 0], "gx", 1),
    ]
    x_down = [
        copy(6, disp.at[0, 0], xv, "gx", -1),
        copy(3, den.at[0:2], xhi.at[0], "gx", -1),
        copy(4, mom.at[2, 0:2], xhi.at[3], "gx", -1),
        copy(5, en.at[1], xhi.at[4, 1], "gx", -1),
    ]
    x_down_half = [
        copy(24, mom.at[0:2, 0:2], xhi.at[1:3], "gx", -1),
        copy(25, en.at[0], xhi.at[4, 0], "gx", -1),
    ]
    up_half = (me < end) & ~(leg_out & odd)
    down_half = (me > 0) & ~(leg_out & (par == 0))
    low_half = (me > 0) & ~(leg_in & (par == 0))
    high_half = (me < end) & ~(leg_in & odd)

    def each(cond, copies, act):
        @pl.when(cond)
        def _():
            for c in copies:
                act(c)

    def go(c):
        c.start()

    hi_rows = slice(top, top + SUB)
    y_up = [
        copy(7, den.at[:, ny - SUB : ny], q.at[0, :, 0:SUB], "gy", 1),
        copy(8, mom.at[:, :, ny - SUB : ny], q.at[1:4, :, 0:SUB], "gy", 1),
        copy(9, en.at[:, ny - SUB : ny], q.at[4, :, 0:SUB], "gy", 1),
    ]
    y_down = [
        copy(10, den.at[:, 0:SUB], q.at[0, :, hi_rows], "gy", -1),
        copy(11, mom.at[:, :, 0:SUB], q.at[1:4, :, hi_rows], "gy", -1),
        copy(12, en.at[:, 0:SUB], q.at[4, :, hi_rows], "gy", -1),
        copy(13, disp.at[1, :, 0:SUB], dy.at[:, hi_rows], "gy", -1),
    ]
    z_up = [copy(14, edge, zlo, "gz", 1)]
    z_down = [copy(15, edge, zhi, "gz", -1)]

    def start(axis, ups, downs):
        @pl.when(pos[axis] < last[axis])
        def _():
            for c in ups:
                c.start()

        @pl.when(pos[axis] > 0)
        def _():
            for c in downs:
                c.start()

    def arrive(axis, ups, downs, fill_low, fill_high):
        @pl.when(pos[axis] > 0)
        def _():
            for c in ups:
                c.wait_recv()

        @pl.when(pos[axis] < last[axis])
        def _():
            for c in downs:
                c.wait_recv()

        @pl.when(pos[axis] == 0)
        def _():
            fill_low()

        @pl.when(pos[axis] == last[axis])
        def _():
            fill_high()

    def sent(axis, ups, downs):
        @pl.when(pos[axis] < last[axis])
        def _():
            for c in ups:
                c.wait_send()

        @pl.when(pos[axis] > 0)
        def _():
            for c in downs:
                c.wait_send()

    each(leg_out, legs, go)
    each(odd & (me < end), x_up, go)
    each(me > 0, x_down, go)
    each((par == 0) & (me < end), x_up, go)
    each(up_half, x_up_half, go)
    each(down_half, x_down_half, go)
    start("gy", y_up, y_down)

    for c in locals_:
        c.wait()

    flag = [flags[i].astype(jnp.float32) for i in range(6)]

    def low_mult(a):
        return jnp.where(pos[AXES[a]] == 0, flag[2 * a], 1.0)

    def high_mult(a):
        return jnp.where(pos[AXES[a]] == last[AXES[a]], flag[2 * a + 1], 1.0)

    def outer_low(a):
        return jnp.where(pos[AXES[a]] == 0, flag[2 * a], 0.0)

    def outer_high(a):
        return jnp.where(pos[AXES[a]] == last[AXES[a]], flag[2 * a + 1], 0.0)

    lane = lax.broadcasted_iota(jnp.int32, (ny, nz), 1)
    row = lax.broadcasted_iota(jnp.int32, (ny, nz), 0)

    def pack(x, carry):
        new = list(carry)
        for f in range(6):
            p = f * nx + x
            k = f * nx // per
            at = 4 * lax.rem(p, per)
            plane = q[f, x, SUB:top] if f < 5 else dz[x].astype(jnp.float32)
            moved = pltpu.roll(plane, at, 1)
            mine = lax.rem(lane + 2 - at + nz, nz) < 4
            new[k] = jnp.where(mine, moved, new[k])
        return tuple(new)

    packed = lax.fori_loop(0, nx, pack, tuple(jnp.zeros((ny, nz), jnp.float32) for _ in range(parts)))
    for k in range(parts):
        edge[k] = packed[k]

    wz = jnp.where(lane == 0, outer_low(2), 0.0) - jnp.where(lane == nz - 1, outer_high(2), 0.0)
    wy = jnp.where(row == 0, outer_low(1), 0.0) - jnp.where(row == ny - 1, outer_high(1), 0.0)
    wx_low, wx_high = outer_low(0), outer_high(0)

    def total(x, carry):
        a, b = carry
        wx = jnp.where(x == 0, wx_low, 0.0) - jnp.where(x == nx - 1, wx_high, 0.0)
        w = 1.0 + scale * (
            wz * dz[x].astype(jnp.float32)
            + wy * dy[x, SUB:top].astype(jnp.float32)
            + wx * dx[x].astype(jnp.float32)
        )
        return (
            a + jnp.sum((q[0, x, SUB:top] * w).reshape(ny // SUB, SUB, nz), 0),
            b + jnp.sum((q[4, x, SUB:top] * w).reshape(ny // SUB, SUB, nz), 0),
        )

    zero = jnp.zeros((SUB, nz), jnp.float32)
    mass, power = lax.fori_loop(0, nx, total, (zero, zero))
    sum_z[pos["gz"], 0] = mass
    sum_z[pos["gz"], 1] = power
    start("gz", z_up, z_down)

    def line(axis, slots, ss, rs):
        count = sizes[axis]
        copies = []
        for o in range(1, count):
            me = pos[axis]
            copies.append(
                pltpu.make_async_remote_copy(
                    src_ref=slots.at[me], dst_ref=slots.at[me], send_sem=ss.at[o],
                    recv_sem=rs.at[me], device_id={axis: lax.rem(me + o, count)},
                    device_id_type=pl.DeviceIdType.MESH,
                )
            )
        return copies

    def collect(axis, slots, ss, rs):
        count = sizes[axis]
        for o in range(1, count):
            peer = lax.rem(pos[axis] + o, count)
            pltpu.make_async_remote_copy(
                src_ref=slots.at[peer], dst_ref=slots.at[peer], send_sem=ss.at[o],
                recv_sem=rs.at[peer], device_id={axis: peer},
                device_id_type=pl.DeviceIdType.MESH,
            ).wait_recv()
        a, b = slots[0, 0], slots[0, 1]
        for o in range(1, count):
            a = a + slots[o, 0]
            b = b + slots[o, 1]
        return a, b

    line_z = line("gz", sum_z, ssz, rsz)
    hops = [
        pltpu.make_async_remote_copy(
            src_ref=sum_y.at[2 * i], dst_ref=sum_y.at[2 * i + 1], send_sem=ssy.at[i],
            recv_sem=rsy.at[i], device_id={"gy": across(stride)},
            device_id_type=pl.DeviceIdType.MESH,
        )
        for i, stride in enumerate(strides)
    ]
    line_y = hops if doubling else line("gy", sum_y, ssy, rsy)

    def step_y(i):
        hops[i].wait_recv()
        a = sum_y[2 * i, 0] + sum_y[2 * i + 1, 0]
        b = sum_y[2 * i, 1] + sum_y[2 * i + 1, 1]
        if i + 1 < len(hops):
            sum_y[2 * i + 2, 0] = a
            sum_y[2 * i + 2, 1] = b
            hops[i + 1].start()
        return a, b

    line_x = line("gx", sum_x, ssx, rsx)
    for c in line_z:
        c.start()

    def z_low():
        e = edge[...]
        zlo[...] = jnp.where(lane3 & 3 == 3, pltpu.roll(e, nz - 1, 2), pltpu.roll(e, nz - 2, 2))

    def z_high():
        e = edge[...]
        zhi[...] = jnp.where(lane3 & 3 == 0, pltpu.roll(e, 1, 2), pltpu.roll(e, 2, 2))

    lane3 = lax.broadcasted_iota(jnp.int32, (parts, ny, nz), 2)
    arrive("gz", z_up, z_down, z_low, z_high)
    low = lane & 3 == 0
    for k in range(parts):
        e, l, h = edge[k], zlo[k], zhi[k]
        r1, r2 = pltpu.roll(l, 1, 1), pltpu.roll(l, 2, 1)
        l1, l2 = pltpu.roll(h, nz - 1, 1), pltpu.roll(h, nz - 2, 1)
        cq[k] = jnp.where(low, r1, l1)
        cs[k] = jnp.where(low, minmod(e - r1, r1 - r2), minmod(l2 - l1, l1 - e))

    first, final = lane == 0, lane == nz - 1
    z_lo_mult = jnp.where(first, low_mult(2), 1.0) * scale
    z_hi_mult = high_mult(2) * scale
    outs = (
        lambda x: out_d.at[x], lambda x: out_m.at[0, x], lambda x: out_m.at[1, x],
        lambda x: out_m.at[2, x], lambda x: out_e.at[x],
    )

    def along_z(x, _):
        v = dz[x].astype(jnp.float32) * z_lo_mult
        g = gain(v)

        def ghosts(ref, f):
            back = lax.rem(nz - 4 * lax.rem(f * nx + x, per), nz)
            return pltpu.roll(ref[f * nx // per], back, 1)

        vh = ghosts(cq, 5) * z_hi_mult
        gh = gain(vh)
        for f in range(5):
            plane = q[f, x, SUB:top]
            gq, gs = ghosts(cq, f), ghosts(cs, f)
            qm = jnp.where(first, gq, pltpu.roll(plane, 1, 1))
            d = plane - qm
            s = minmod(jnp.where(final, gq - plane, pltpu.roll(d, nz - 1, 1)), d)
            sm = jnp.where(first, gs, pltpu.roll(s, 1, 1))
            fl = flux(v, g, qm, plane, sm, s)
            fh = jnp.where(final, flux(vh, gh, plane, gq, s, gs), pltpu.roll(fl, nz - 1, 1))
            outs[f](x)[...] = plane + (fl - fh)
        return 0

    lax.fori_loop(0, nx, along_z, 0)

    @pl.when(relays)
    def _():
        for a, b in zip(legs, onward):
            a.wait_recv()
            b.start()

    a, b = collect("gz", sum_z, ssz, rsz)
    own = 0 if doubling else pos["gy"]
    sum_y[own, 0] = a
    sum_y[own, 1] = b

    def y_low():
        q[:, :, 0:SUB] = jnp.broadcast_to(q[:, :, SUB : SUB + 1], (5, nx, SUB, nz))

    def y_high():
        q[:, :, hi_rows] = jnp.broadcast_to(q[:, :, top - 1 : top], (5, nx, SUB, nz))
        dy[:, hi_rows] = jnp.broadcast_to(dy[:, top - 1 : top], (nx, SUB, nz))

    arrive("gy", y_up, y_down, y_low, y_high)
    for c in line_y[:1] if doubling else line_y:
        c.start()
    tall = ny + 2 * SUB
    rows = lax.broadcasted_iota(jnp.int32, (tall, nz), 0)
    inside = (rows >= SUB) & (rows <= top)
    y_mult = jnp.where(
        rows == SUB, low_mult(1) * scale, jnp.where(rows == top, high_mult(1) * scale, scale)
    )

    def along_y(x, _):
        v = jnp.where(inside, dy[x].astype(jnp.float32), 0.0) * y_mult
        g = gain(v)
        for f in range(5):
            plane = q[f, x]
            qm = pltpu.roll(plane, 1, 0)
            d = plane - qm
            s = minmod(pltpu.roll(d, tall - 1, 0), d)
            fl = flux(v, g, qm, plane, pltpu.roll(s, 1, 0), s)
            ch = fl - pltpu.roll(fl, tall - 1, 0)
            outs[f](x)[...] += ch[SUB:top]
        return 0

    lax.fori_loop(0, nx, along_y, 0)

    if hops:
        a, b = step_y(0)

    def core(r, _):
        at = pl.ds(pl.multiple_of(r * SUB, SUB), SUB)
        inner = pl.ds(pl.multiple_of(r * SUB + SUB, SUB), SUB)
        vs = [dx[c, at].astype(jnp.float32) * scale for c in range(2, nx - 1)]
        gs = [gain(v) for v in vs]
        for f in range(5):
            line_q = [q[f, c, inner] for c in range(nx)]
            ds = [line_q[i + 1] - line_q[i] for i in range(nx - 1)]
            ss = [minmod(ds[i + 1], ds[i]) for i in range(nx - 2)]
            fl = [
                flux(vs[i], gs[i], line_q[i + 1], line_q[i + 2], ss[i], ss[i + 1])
                for i in range(nx - 3)
            ]
            for c in range(1, nx - 1):
                change = fl[c - 2] if c >= 2 else 0.0
                ref = outs[f](c)
                ref[at] += change - fl[c - 1] if c < nx - 2 else change
        return 0

    lax.fori_loop(0, ny // SUB, core, 0)

    def x_low():
        xlo[...] = jnp.broadcast_to(q[:, 0:1, SUB:top], (5, 2, ny, nz))

    def x_high():
        xhi[...] = jnp.broadcast_to(q[:, nx - 1 : nx, SUB:top], (5, 2, ny, nz))
        xv[...] = dx[nx - 1]

    if not doubling:
        a, b = collect("gy", sum_y, ssy, rsy)
    for i in range(1, len(hops)):
        a, b = step_y(i)
    sum_x[pos["gx"], 0] = a
    sum_x[pos["gx"], 1] = b
    for c in line_x:
        c.start()
    arrive("gx", x_up, x_down, x_low, x_high)
    x_lo_mult, x_hi_mult = low_mult(0) * scale, high_mult(0) * scale

    def x_rows(r):
        return pl.ds(pl.multiple_of(r * SUB, SUB), SUB), pl.ds(
            pl.multiple_of(r * SUB + SUB, SUB), SUB
        )

    def x_flux(v, g, cells4):
        ds = [cells4[i + 1] - cells4[i] for i in range(3)]
        return flux(
            v, g, cells4[1], cells4[2], minmod(ds[1], ds[0]), minmod(ds[2], ds[1])
        )

    def rim(fields, r, _):
        at, inner = x_rows(r)
        faces = (0, 1, nx - 1, nx)
        vs = [
            dx[0, at].astype(jnp.float32) * x_lo_mult,
            dx[1, at].astype(jnp.float32) * scale,
            dx[nx - 1, at].astype(jnp.float32) * scale,
            xv[at].astype(jnp.float32) * x_hi_mult,
        ]
        gs = [gain(v) for v in vs]
        for f in fields:
            a = [xlo[f, 0, at], xlo[f, 1, at]] + [q[f, c, inner] for c in range(3)]
            b = [q[f, c, inner] for c in range(nx - 3, nx)] + [xhi[f, 0, at], xhi[f, 1, at]]
            fl = [x_flux(vs[i], gs[i], (a, a, b, b)[i][i % 2 : i % 2 + 4]) for i in range(4)]
            for c, change in (
                (0, fl[0] - fl[1]), (1, fl[1]), (nx - 2, -fl[2]), (nx - 1, fl[2] - fl[3]),
            ):
                ref = outs[f](c)
                ref[at] += change
        return 0

    lax.fori_loop(0, ny // SUB, functools.partial(rim, (0, 3)), 0)
    each(low_half, x_up_half, lambda c: c.wait_recv())
    each(high_half, x_down_half, lambda c: c.wait_recv())
    each(leg_in, landed, lambda c: c.wait_recv())
    lax.fori_loop(0, ny // SUB, functools.partial(rim, (1, 2, 4)), 0)

    a, b = collect("gx", sum_x, ssx, rsx)
    sums[0] = a
    sums[1] = b
    sent("gx", x_up, x_down)
    each(leg_out, legs, lambda c: c.wait_send())
    each(relays, onward, lambda c: c.wait_send())
    each(up_half, x_up_half, lambda c: c.wait_send())
    each(down_half, x_down_half, lambda c: c.wait_send())
    sent("gy", y_up, y_down)
    sent("gz", z_up, z_down)
    for c in line_x + line_y + line_z:
        c.wait_send()


def put(cells, den, mom, en, sums, out_d, out_m, out_e, totals, sem):
    pairs = [(den, out_d), (en, out_e)] + [(mom.at[c], out_m.at[c]) for c in range(3)]
    half = den.shape[0] // 2
    pairs = [
        (src.at[at], dst.at[at])
        for src, dst in pairs
        for at in (slice(0, half), slice(half, 2 * half))
    ]
    moves = [
        pltpu.make_async_copy(src, dst, sem.at[i]) for i, (src, dst) in enumerate(pairs)
    ]
    for c in moves:
        c.start()
    totals[0] = jnp.sum(sums[0]) / cells
    totals[1] = jnp.sum(sums[1]) / cells
    for c in moves:
        c.wait()


def shards(density, momentum, energy, displacement, flags):
    sizes = {a: lax.axis_size(a) for a in AXES}
    nx, ny, nz = density.shape
    tall = ny + 2 * SUB
    per = nz // 4
    parts = -(-6 * nx // per)
    f32, i32 = jnp.float32, jnp.int32
    dma = pltpu.SemaphoreType.DMA
    any_ = pl.BlockSpec(memory_space=pl.ANY)
    hbm = pl.BlockSpec(memory_space=pltpu.HBM)
    vmem = pl.BlockSpec(memory_space=pltpu.VMEM)
    smem = pl.BlockSpec(memory_space=pltpu.SMEM)
    cells = float(nx * ny * nz)
    for a in AXES:
        cells = cells * sizes[a]
    outputs = tuple(jax.ShapeDtypeStruct(v.shape, f32) for v in (density, momentum, energy))
    results = pl.pallas_call(
        functools.partial(kernel, sizes),
        out_shape=outputs + (jax.ShapeDtypeStruct((2, SUB, nz), f32),),
        in_specs=[hbm] * 5,
        out_specs=(vmem, vmem, vmem, vmem),
        scratch_shapes=[
            pltpu.SMEM((6,), i32),
            pltpu.VMEM((5, nx, tall, nz), f32),
            pltpu.VMEM((nx, ny, nz), i32),
            pltpu.VMEM((nx, tall, nz), i32),
            pltpu.VMEM((nx, ny, nz), i32),
            pltpu.VMEM((2, 5, 2, ny, nz), f32),
            pltpu.VMEM((5, ny, nz), f32),
            pltpu.VMEM((ny, nz), i32),
        ]
        + [pltpu.VMEM((parts, ny, nz), f32) for _ in range(5)]
        + [pltpu.VMEM((sizes[a], 2, SUB, nz), f32) for a in AXES]
        + [dma((7,)), dma((26,)), dma((26,))]
        + [dma((sizes[a],)) for a in AXES for _ in range(2)],
        compiler_params=pltpu.CompilerParams(
            collective_id=0, has_side_effects=True, vmem_limit_bytes=12 << 20
        ),
    )(
        *(
            pltpu.with_memory_space_constraint(v, pltpu.HBM)
            for v in (flags, density, momentum, energy, displacement)
        )
    )
    return pl.pallas_call(
        functools.partial(put, cells),
        out_shape=outputs + (jax.ShapeDtypeStruct((2,), f32),),
        in_specs=[any_, any_, any_, vmem],
        out_specs=(hbm, hbm, hbm, smem),
        scratch_shapes=[dma((10,))],
        compiler_params=pltpu.CompilerParams(vmem_limit_bytes=2 << 20),
    )(*results)


def solution(mesh):
    return jax.shard_map(
        shards,
        mesh=mesh,
        in_specs=(
            P("gx", "gy", "gz"),
            P(None, "gx", "gy", "gz"),
            P("gx", "gy", "gz"),
            P(None, "gx", "gy", "gz"),
            P(),
        ),
        out_specs=(P("gx", "gy", "gz"), P(None, "gx", "gy", "gz"), P("gx", "gy", "gz"), P()),
        check_vma=False,
    )
```

```python
import functools

import jax
import jax.numpy as jnp
from jax import lax
from jax.experimental import pallas as pl
from jax.experimental.pallas import tpu as pltpu
from jax.sharding import PartitionSpec as P

AXES = ("gx", "gy", "gz")
SUB = 8


def minmod(p, r):
    return jnp.maximum(jnp.minimum(r, 0.0), jnp.minimum(p, jnp.maximum(r, 0.0)))


def gain(v):
    size = jnp.abs(v)
    return 0.5 * size * (1.0 - size)


def flux(v, g, q_low, q_high, s_low, s_high):
    up = v > 0
    return v * jnp.where(up, q_low, q_high) + g * jnp.where(up, s_low, s_high)


def kernel(
    sizes, flags_in, den, mom, en, disp, out_d, out_m, out_e, sums,
    flags, q, dx, dy, dz, xh, hop, xv, edge, zlo, zhi, cq, cs, sum_x, sum_y, sum_z,
    local_sem, send_sem, recv_sem, ssx, rsx, ssy, rsy, ssz, rsz,
):
    nx, ny, nz = den.shape
    pos = {a: lax.axis_index(a) for a in AXES}
    top = ny + SUB
    per = nz // 4
    parts = edge.shape[0]
    scale = 1.0 / 256.0
    xlo, xhi = xh.at[0], xh.at[1]

    barrier = pltpu.get_barrier_semaphore()
    greeted = 0
    for a in ("gy", "gx", "gz"):
        for o in range(1, sizes[a]):
            peer = lax.rem(pos[a] + o, sizes[a])
            pl.semaphore_signal(
                barrier, inc=1, device_id={a: peer}, device_id_type=pl.DeviceIdType.MESH
            )
            greeted += 1

    locals_ = [
        pltpu.make_async_copy(den, q.at[0, :, SUB:top], local_sem.at[0]),
        pltpu.make_async_copy(mom, q.at[1:4, :, SUB:top], local_sem.at[1]),
        pltpu.make_async_copy(en, q.at[4, :, SUB:top], local_sem.at[2]),
        pltpu.make_async_copy(disp.at[2], dz, local_sem.at[3]),
        pltpu.make_async_copy(disp.at[1], dy.at[:, SUB:top], local_sem.at[4]),
        pltpu.make_async_copy(disp.at[0], dx, local_sem.at[5]),
        pltpu.make_async_copy(flags_in, flags, local_sem.at[6]),
    ]
    for c in locals_:
        c.start()

    pl.semaphore_wait(barrier, greeted)

    def copy(k, src, dst, axis, step):
        return pltpu.make_async_remote_copy(
            src_ref=src, dst_ref=dst, send_sem=send_sem.at[k], recv_sem=recv_sem.at[k],
            device_id={axis: pos[axis] + step}, device_id_type=pl.DeviceIdType.MESH,
        )

    last = {a: sizes[a] - 1 for a in AXES}
    me = pos["gx"]
    par = lax.rem(me, 2)
    odd = par == 1
    end = last["gx"]
    leg_out = (odd & (me + 2 <= end)) | ((par == 0) & (me >= 2))
    relays = (odd & (me >= 3)) | ((par == 0) & (me + 2 <= end))
    leg_in = (me + 1 <= end) & (odd | (me >= 2))
    begin = par * (nx - 2)
    other = 1 - par

    def remote(k, src, dst, target):
        return pltpu.make_async_remote_copy(
            src_ref=src, dst_ref=dst, send_sem=send_sem.at[k], recv_sem=recv_sem.at[k],
            device_id={"gx": target}, device_id_type=pl.DeviceIdType.MESH,
        )

    over = me + 4 * par - 2
    legs = [
        remote(16, mom.at[0, pl.ds(begin, 2)], hop.at[0:2], over),
        remote(17, mom.at[1, pl.ds(begin, 2)], hop.at[2:4], over),
        remote(18, en.at[begin], hop.at[4], over),
    ]
    beside = me + 1 - 2 * par
    onward = [
        remote(19, hop.at[0:2], xh.at[other, 1], beside),
        remote(20, hop.at[2:4], xh.at[other, 2], beside),
        remote(21, hop.at[4], xh.at[other, 4, 0], beside),
    ]
    landed = [
        remote(19, hop.at[0:2], xh.at[par, 1], beside),
        remote(20, hop.at[2:4], xh.at[par, 2], beside),
        remote(21, hop.at[4], xh.at[par, 4, 0], beside),
    ]
    x_up = [
        copy(0, den.at[nx - 2 : nx], xlo.at[0], "gx", 1),
        copy(1, mom.at[2, nx - 2 : nx], xlo.at[3], "gx", 1),
        copy(2, en.at[nx - 1], xlo.at[4, 1], "gx", 1),
    ]
    x_up_half = [
        copy(22, mom.at[0:2, nx - 2 : nx], xlo.at[1:3], "gx", 1),
        copy(23, en.at[nx - 2], xlo.at[4, 0], "gx", 1),
    ]
    x_down = [
        copy(6, disp.at[0, 0], xv, "gx", -1),
        copy(3, den.at[0:2], xhi.at[0], "gx", -1),
        copy(4, mom.at[2, 0:2], xhi.at[3], "gx", -1),
        copy(5, en.at[1], xhi.at[4, 1], "gx", -1),
    ]
    x_down_half = [
        copy(24, mom.at[0:2, 0:2], xhi.at[1:3], "gx", -1),
        copy(25, en.at[0], xhi.at[4, 0], "gx", -1),
    ]
    up_half = (me < end) & ~(leg_out & odd)
    down_half = (me > 0) & ~(leg_out & (par == 0))
    low_half = (me > 0) & ~(leg_in & (par == 0))
    high_half = (me < end) & ~(leg_in & odd)

    def each(cond, copies, act):
        @pl.when(cond)
        def _():
            for c in copies:
                act(c)

    def go(c):
        c.start()

    hi_rows = slice(top, top + SUB)
    y_up = [
        copy(7, den.at[:, ny - SUB : ny], q.at[0, :, 0:SUB], "gy", 1),
        copy(8, mom.at[:, :, ny - SUB : ny], q.at[1:4, :, 0:SUB], "gy", 1),
        copy(9, en.at[:, ny - SUB : ny], q.at[4, :, 0:SUB], "gy", 1),
    ]
    y_down = [
        copy(10, den.at[:, 0:SUB], q.at[0, :, hi_rows], "gy", -1),
        copy(11, mom.at[:, :, 0:SUB], q.at[1:4, :, hi_rows], "gy", -1),
        copy(12, en.at[:, 0:SUB], q.at[4, :, hi_rows], "gy", -1),
        copy(13, disp.at[1, :, 0:SUB], dy.at[:, hi_rows], "gy", -1),
    ]
    z_up = [copy(14, edge, zlo, "gz", 1)]
    z_down = [copy(15, edge, zhi, "gz", -1)]

    def start(axis, ups, downs):
        @pl.when(pos[axis] < last[axis])
        def _():
            for c in ups:
                c.start()

        @pl.when(pos[axis] > 0)
        def _():
            for c in downs:
                c.start()

    def arrive(axis, ups, downs, fill_low, fill_high):
        @pl.when(pos[axis] > 0)
        def _():
            for c in ups:
                c.wait_recv()

        @pl.when(pos[axis] < last[axis])
        def _():
            for c in downs:
                c.wait_recv()

        @pl.when(pos[axis] == 0)
        def _():
            fill_low()

        @pl.when(pos[axis] == last[axis])
        def _():
            fill_high()

    def sent(axis, ups, downs):
        @pl.when(pos[axis] < last[axis])
        def _():
            for c in ups:
                c.wait_send()

        @pl.when(pos[axis] > 0)
        def _():
            for c in downs:
                c.wait_send()

    each(leg_out, legs, go)
    each(odd & (me < end), x_up, go)
    each(me > 0, x_down, go)
    each((par == 0) & (me < end), x_up, go)
    each(up_half, x_up_half, go)
    each(down_half, x_down_half, go)
    start("gy", y_up, y_down)

    for c in locals_:
        c.wait()

    flag = [flags[i].astype(jnp.float32) for i in range(6)]

    def low_mult(a):
        return jnp.where(pos[AXES[a]] == 0, flag[2 * a], 1.0)

    def high_mult(a):
        return jnp.where(pos[AXES[a]] == last[AXES[a]], flag[2 * a + 1], 1.0)

    def outer_low(a):
        return jnp.where(pos[AXES[a]] == 0, flag[2 * a], 0.0)

    def outer_high(a):
        return jnp.where(pos[AXES[a]] == last[AXES[a]], flag[2 * a + 1], 0.0)

    lane = lax.broadcasted_iota(jnp.int32, (ny, nz), 1)
    row = lax.broadcasted_iota(jnp.int32, (ny, nz), 0)

    def pack(x, carry):
        new = list(carry)
        for f in range(6):
            p = f * nx + x
            k = f * nx // per
            at = 4 * lax.rem(p, per)
            plane = q[f, x, SUB:top] if f < 5 else dz[x].astype(jnp.float32)
            moved = pltpu.roll(plane, at, 1)
            mine = lax.rem(lane + 2 - at + nz, nz) < 4
            new[k] = jnp.where(mine, moved, new[k])
        return tuple(new)

    packed = lax.fori_loop(0, nx, pack, tuple(jnp.zeros((ny, nz), jnp.float32) for _ in range(parts)))
    for k in range(parts):
        edge[k] = packed[k]

    wz = jnp.where(lane == 0, outer_low(2), 0.0) - jnp.where(lane == nz - 1, outer_high(2), 0.0)
    wy = jnp.where(row == 0, outer_low(1), 0.0) - jnp.where(row == ny - 1, outer_high(1), 0.0)
    wx_low, wx_high = outer_low(0), outer_high(0)

    def total(x, carry):
        a, b = carry
        wx = jnp.where(x == 0, wx_low, 0.0) - jnp.where(x == nx - 1, wx_high, 0.0)
        w = 1.0 + scale * (
            wz * dz[x].astype(jnp.float32)
            + wy * dy[x, SUB:top].astype(jnp.float32)
            + wx * dx[x].astype(jnp.float32)
        )
        return (
            a + jnp.sum((q[0, x, SUB:top] * w).reshape(ny // SUB, SUB, nz), 0),
            b + jnp.sum((q[4, x, SUB:top] * w).reshape(ny // SUB, SUB, nz), 0),
        )

    zero = jnp.zeros((SUB, nz), jnp.float32)
    mass, power = lax.fori_loop(0, nx, total, (zero, zero))
    sum_z[pos["gz"], 0] = mass
    sum_z[pos["gz"], 1] = power
    start("gz", z_up, z_down)

    def line(axis, slots, ss, rs):
        count = sizes[axis]
        copies = []
        for o in range(1, count):
            me = pos[axis]
            copies.append(
                pltpu.make_async_remote_copy(
                    src_ref=slots.at[me], dst_ref=slots.at[me], send_sem=ss.at[o],
                    recv_sem=rs.at[me], device_id={axis: lax.rem(me + o, count)},
                    device_id_type=pl.DeviceIdType.MESH,
                )
            )
        return copies

    def collect(axis, slots, ss, rs):
        count = sizes[axis]
        for o in range(1, count):
            peer = lax.rem(pos[axis] + o, count)
            pltpu.make_async_remote_copy(
                src_ref=slots.at[peer], dst_ref=slots.at[peer], send_sem=ss.at[o],
                recv_sem=rs.at[peer], device_id={axis: peer},
                device_id_type=pl.DeviceIdType.MESH,
            ).wait_recv()
        a, b = slots[0, 0], slots[0, 1]
        for o in range(1, count):
            a = a + slots[o, 0]
            b = b + slots[o, 1]
        return a, b

    line_z = line("gz", sum_z, ssz, rsz)
    line_y = line("gy", sum_y, ssy, rsy)
    line_x = line("gx", sum_x, ssx, rsx)
    for c in line_z:
        c.start()

    def z_low():
        e = edge[...]
        zlo[...] = jnp.where(lane3 & 3 == 3, pltpu.roll(e, nz - 1, 2), pltpu.roll(e, nz - 2, 2))

    def z_high():
        e = edge[...]
        zhi[...] = jnp.where(lane3 & 3 == 0, pltpu.roll(e, 1, 2), pltpu.roll(e, 2, 2))

    lane3 = lax.broadcasted_iota(jnp.int32, (parts, ny, nz), 2)
    arrive("gz", z_up, z_down, z_low, z_high)
    low = lane & 3 == 0
    for k in range(parts):
        e, l, h = edge[k], zlo[k], zhi[k]
        r1, r2 = pltpu.roll(l, 1, 1), pltpu.roll(l, 2, 1)
        l1, l2 = pltpu.roll(h, nz - 1, 1), pltpu.roll(h, nz - 2, 1)
        cq[k] = jnp.where(low, r1, l1)
        cs[k] = jnp.where(low, minmod(e - r1, r1 - r2), minmod(l2 - l1, l1 - e))

    first, final = lane == 0, lane == nz - 1
    z_lo_mult = jnp.where(first, low_mult(2), 1.0) * scale
    z_hi_mult = high_mult(2) * scale
    outs = (
        lambda x: out_d.at[x], lambda x: out_m.at[0, x], lambda x: out_m.at[1, x],
        lambda x: out_m.at[2, x], lambda x: out_e.at[x],
    )

    def along_z(x, _):
        v = dz[x].astype(jnp.float32) * z_lo_mult
        g = gain(v)

        def ghosts(ref, f):
            back = lax.rem(nz - 4 * lax.rem(f * nx + x, per), nz)
            return pltpu.roll(ref[f * nx // per], back, 1)

        vh = ghosts(cq, 5) * z_hi_mult
        gh = gain(vh)
        for f in range(5):
            plane = q[f, x, SUB:top]
            gq, gs = ghosts(cq, f), ghosts(cs, f)
            qm = jnp.where(first, gq, pltpu.roll(plane, 1, 1))
            d = plane - qm
            s = minmod(jnp.where(final, gq - plane, pltpu.roll(d, nz - 1, 1)), d)
            sm = jnp.where(first, gs, pltpu.roll(s, 1, 1))
            fl = flux(v, g, qm, plane, sm, s)
            fh = jnp.where(final, flux(vh, gh, plane, gq, s, gs), pltpu.roll(fl, nz - 1, 1))
            outs[f](x)[...] = plane + (fl - fh)
        return 0

    lax.fori_loop(0, nx, along_z, 0)

    @pl.when(relays)
    def _():
        for a, b in zip(legs, onward):
            a.wait_recv()
            b.start()

    a, b = collect("gz", sum_z, ssz, rsz)
    sum_y[pos["gy"], 0] = a
    sum_y[pos["gy"], 1] = b

    def y_low():
        q[:, :, 0:SUB] = jnp.broadcast_to(q[:, :, SUB : SUB + 1], (5, nx, SUB, nz))

    def y_high():
        q[:, :, hi_rows] = jnp.broadcast_to(q[:, :, top - 1 : top], (5, nx, SUB, nz))
        dy[:, hi_rows] = jnp.broadcast_to(dy[:, top - 1 : top], (nx, SUB, nz))

    arrive("gy", y_up, y_down, y_low, y_high)
    for c in line_y:
        c.start()
    tall = ny + 2 * SUB
    rows = lax.broadcasted_iota(jnp.int32, (tall, nz), 0)
    inside = (rows >= SUB) & (rows <= top)
    y_mult = jnp.where(
        rows == SUB, low_mult(1) * scale, jnp.where(rows == top, high_mult(1) * scale, scale)
    )

    def along_y(x, _):
        v = jnp.where(inside, dy[x].astype(jnp.float32), 0.0) * y_mult
        g = gain(v)
        for f in range(5):
            plane = q[f, x]
            qm = pltpu.roll(plane, 1, 0)
            d = plane - qm
            s = minmod(pltpu.roll(d, tall - 1, 0), d)
            fl = flux(v, g, qm, plane, pltpu.roll(s, 1, 0), s)
            ch = fl - pltpu.roll(fl, tall - 1, 0)
            outs[f](x)[...] += ch[SUB:top]
        return 0

    lax.fori_loop(0, nx, along_y, 0)

    a, b = collect("gy", sum_y, ssy, rsy)
    sum_x[pos["gx"], 0] = a
    sum_x[pos["gx"], 1] = b

    def core(r, _):
        at = pl.ds(pl.multiple_of(r * SUB, SUB), SUB)
        inner = pl.ds(pl.multiple_of(r * SUB + SUB, SUB), SUB)
        vs = [dx[c, at].astype(jnp.float32) * scale for c in range(2, nx - 1)]
        gs = [gain(v) for v in vs]
        for f in range(5):
            line_q = [q[f, c, inner] for c in range(nx)]
            ds = [line_q[i + 1] - line_q[i] for i in range(nx - 1)]
            ss = [minmod(ds[i + 1], ds[i]) for i in range(nx - 2)]
            fl = [
                flux(vs[i], gs[i], line_q[i + 1], line_q[i + 2], ss[i], ss[i + 1])
                for i in range(nx - 3)
            ]
            for c in range(1, nx - 1):
                change = fl[c - 2] if c >= 2 else 0.0
                ref = outs[f](c)
                ref[at] += change - fl[c - 1] if c < nx - 2 else change
        return 0

    lax.fori_loop(0, ny // SUB, core, 0)

    def x_low():
        xlo[...] = jnp.broadcast_to(q[:, 0:1, SUB:top], (5, 2, ny, nz))

    def x_high():
        xhi[...] = jnp.broadcast_to(q[:, nx - 1 : nx, SUB:top], (5, 2, ny, nz))
        xv[...] = dx[nx - 1]

    for c in line_x:
        c.start()
    arrive("gx", x_up, x_down, x_low, x_high)
    x_lo_mult, x_hi_mult = low_mult(0) * scale, high_mult(0) * scale

    def x_rows(r):
        return pl.ds(pl.multiple_of(r * SUB, SUB), SUB), pl.ds(
            pl.multiple_of(r * SUB + SUB, SUB), SUB
        )

    def x_flux(v, g, cells4):
        ds = [cells4[i + 1] - cells4[i] for i in range(3)]
        return flux(
            v, g, cells4[1], cells4[2], minmod(ds[1], ds[0]), minmod(ds[2], ds[1])
        )

    def rim(fields, r, _):
        at, inner = x_rows(r)
        faces = (0, 1, nx - 1, nx)
        vs = [
            dx[0, at].astype(jnp.float32) * x_lo_mult,
            dx[1, at].astype(jnp.float32) * scale,
            dx[nx - 1, at].astype(jnp.float32) * scale,
            xv[at].astype(jnp.float32) * x_hi_mult,
        ]
        gs = [gain(v) for v in vs]
        for f in fields:
            a = [xlo[f, 0, at], xlo[f, 1, at]] + [q[f, c, inner] for c in range(3)]
            b = [q[f, c, inner] for c in range(nx - 3, nx)] + [xhi[f, 0, at], xhi[f, 1, at]]
            fl = [x_flux(vs[i], gs[i], (a, a, b, b)[i][i % 2 : i % 2 + 4]) for i in range(4)]
            for c, change in (
                (0, fl[0] - fl[1]), (1, fl[1]), (nx - 2, -fl[2]), (nx - 1, fl[2] - fl[3]),
            ):
                ref = outs[f](c)
                ref[at] += change
        return 0

    lax.fori_loop(0, ny // SUB, functools.partial(rim, (0, 3)), 0)
    for part, whole, fields in ((0, (0,), (1,)), (1, (), (2,)), (2, (1,), (4,))):
        each(low_half, [x_up_half[k] for k in whole], lambda c: c.wait_recv())
        each(high_half, [x_down_half[k] for k in whole], lambda c: c.wait_recv())
        each(leg_in, landed[part : part + 1], lambda c: c.wait_recv())
        lax.fori_loop(0, ny // SUB, functools.partial(rim, fields), 0)

    a, b = collect("gx", sum_x, ssx, rsx)
    sums[0] = a
    sums[1] = b
    sent("gx", x_up, x_down)
    each(leg_out, legs, lambda c: c.wait_send())
    each(relays, onward, lambda c: c.wait_send())
    each(up_half, x_up_half, lambda c: c.wait_send())
    each(down_half, x_down_half, lambda c: c.wait_send())
    sent("gy", y_up, y_down)
    sent("gz", z_up, z_down)
    for c in line_x + line_y + line_z:
        c.wait_send()


def put(cells, den, mom, en, sums, out_d, out_m, out_e, totals, sem):
    pairs = ((mom, out_m), (den, out_d), (en, out_e))
    moves = [
        pltpu.make_async_copy(src, dst, sem.at[i]) for i, (src, dst) in enumerate(pairs)
    ]
    for c in moves:
        c.start()
    totals[0] = jnp.sum(sums[0]) / cells
    totals[1] = jnp.sum(sums[1]) / cells
    for c in moves:
        c.wait()


def shards(density, momentum, energy, displacement, flags):
    sizes = {a: lax.axis_size(a) for a in AXES}
    nx, ny, nz = density.shape
    tall = ny + 2 * SUB
    per = nz // 4
    parts = -(-6 * nx // per)
    f32, i32 = jnp.float32, jnp.int32
    dma = pltpu.SemaphoreType.DMA
    any_ = pl.BlockSpec(memory_space=pl.ANY)
    hbm = pl.BlockSpec(memory_space=pltpu.HBM)
    vmem = pl.BlockSpec(memory_space=pltpu.VMEM)
    smem = pl.BlockSpec(memory_space=pltpu.SMEM)
    cells = float(nx * ny * nz)
    for a in AXES:
        cells = cells * sizes[a]
    outputs = tuple(jax.ShapeDtypeStruct(v.shape, f32) for v in (density, momentum, energy))
    results = pl.pallas_call(
        functools.partial(kernel, sizes),
        out_shape=outputs + (jax.ShapeDtypeStruct((2, SUB, nz), f32),),
        in_specs=[hbm] * 5,
        out_specs=(vmem, vmem, vmem, vmem),
        scratch_shapes=[
            pltpu.SMEM((6,), i32),
            pltpu.VMEM((5, nx, tall, nz), f32),
            pltpu.VMEM((nx, ny, nz), i32),
            pltpu.VMEM((nx, tall, nz), i32),
            pltpu.VMEM((nx, ny, nz), i32),
            pltpu.VMEM((2, 5, 2, ny, nz), f32),
            pltpu.VMEM((5, ny, nz), f32),
            pltpu.VMEM((ny, nz), i32),
        ]
        + [pltpu.VMEM((parts, ny, nz), f32) for _ in range(5)]
        + [pltpu.VMEM((sizes[a], 2, SUB, nz), f32) for a in AXES]
        + [dma((7,)), dma((26,)), dma((26,))]
        + [dma((sizes[a],)) for a in AXES for _ in range(2)],
        compiler_params=pltpu.CompilerParams(
            collective_id=0, has_side_effects=True, vmem_limit_bytes=12 << 20
        ),
    )(
        *(
            pltpu.with_memory_space_constraint(v, pltpu.HBM)
            for v in (flags, density, momentum, energy, displacement)
        )
    )
    return pl.pallas_call(
        functools.partial(put, cells),
        out_shape=outputs + (jax.ShapeDtypeStruct((2,), f32),),
        in_specs=[any_, any_, any_, vmem],
        out_specs=(hbm, hbm, hbm, smem),
        scratch_shapes=[dma((3,))],
        compiler_params=pltpu.CompilerParams(vmem_limit_bytes=2 << 20),
    )(*results)


def solution(mesh):
    return jax.shard_map(
        shards,
        mesh=mesh,
        in_specs=(
            P("gx", "gy", "gz"),
            P(None, "gx", "gy", "gz"),
            P("gx", "gy", "gz"),
            P(None, "gx", "gy", "gz"),
            P(),
        ),
        out_specs=(P("gx", "gy", "gz"), P(None, "gx", "gy", "gz"), P("gx", "gy", "gz"), P()),
        check_vma=False,
    )
```
